32 devices in a mesh: groups: 2 (over y), ctx: 8 (over z, x), head: 2 (over core).
Axes of the slice: x: 2, y: 2, z: 4, core: 2. Of those that a mesh axis runs over, the one named last changes fastest.
Arguments:
- queries: bfloat16 [16, 128, 64, 192], P(('groups', 'ctx'), None, 'head'), parts along dimension 0, may hold values from -360 to 360
- latent_pages: bfloat16 [16, 8, 64, 576], P(('groups', 'ctx'), 'head'), parts along dimension 0, may hold values from -6 to 6
- page_scales: bfloat16 [16, 8, 4, 64], P(('groups', 'ctx'), 'head'), parts along dimension 0, may hold values from 0.5 to 2
- page_table: int32 [16, 8], P(('groups', 'ctx')), parts along dimension 0, may hold values from 0 to 7, each once within a row
- lengths: int32 [16], P(('groups', 'ctx')), parts along dimension 0, may hold values from 128 to 512, as said below
- w_keys: bfloat16 [512, 64, 128], P('ctx', 'head'), may hold values from -0.5 to 0.5
- w_values: bfloat16 [512, 64, 128], P('ctx', 'head'), may hold values from -1 to 1
Outputs:
- attended: bfloat16 [16, 128, 64, 128], P(('groups', 'ctx'), None, 'head'), parts along dimension 0
The draws below stay inside these ranges and needn't reach their ends.
There are 2 independent parts, one for each index of `groups`. The reference program is written for one: setup_inputs(seed, part) draws one part's arguments, and reference() takes and returns one part's arrays. A program takes and returns all parts, laid end to end along the dimension named above; an argument that names none is the same for every part. Nothing has to cross between parts.
Inputs may be any that keep to these rules, and one draw needn't show every extreme that they name: `page_table`: each row is a permutation of 0 to 7. `lengths`: a length counts the cached tokens and the 128 rows of the span, which take the last positions; the longest request of a part has exactly 512 tokens.
All inputs are finite; a program needn't handle non-finite values.
Results may differ from the reference program's by a relative error of at most 0.0084.
Values may be sent and summed in bfloat16 or wider, within the bound.
A program may use at most 64 MiB of HBM per device.

```python
import math
import jax
import jax.numpy as jnp
from jax import lax

HEADS = 64
NOPE = 128
ROPE = 64
VDIM = 128
LATENT = 512
GROUPS = 4
PAGE = 64
SPAN = 128
PAGES_REQ = 8
REQS = 8


def draw_latent_pages(key, part):
    code_key = jax.random.fold_in(key, 202)
    rope_key = jax.random.fold_in(key, 303)
    code_values = jnp.clip(jax.random.normal(code_key, (REQS, PAGES_REQ, PAGE, LATENT), jnp.float32), -6.0, 6.0)
    rotary = jnp.clip(jax.random.normal(rope_key, (REQS, PAGES_REQ, PAGE, ROPE), jnp.float32), -4.0, 4.0)
    return jnp.concatenate([code_values, rotary], axis=-1).astype(jnp.bfloat16)


def draw_queries(key, part):
    full_shape = (REQS, SPAN, HEADS, NOPE + ROPE)
    main_key = jax.random.fold_in(key, 404)
    drawn = jnp.clip(jax.random.normal(main_key, full_shape, jnp.float32), -6.0, 6.0)
    return drawn.astype(jnp.bfloat16)


def draw_lengths(key, part):
    longest_tokens = PAGES_REQ * PAGE
    reach = longest_tokens - SPAN + 1
    first_key = jax.random.fold_in(key, 606)
    second_key = jax.random.fold_in(key, 707)
    third_key = jax.random.fold_in(key, 808)
    first_draw = jax.random.randint(first_key, (REQS,), 0, reach, jnp.int32)
    second_draw = jax.random.randint(second_key, (REQS,), 0, reach, jnp.int32)
    extra_tokens = first_draw * second_draw // reach
    chosen_request = jax.random.randint(third_key, (), 0, REQS, jnp.int32)
    result = SPAN + extra_tokens
    return result.at[chosen_request].set(longest_tokens)


def steps_of(stream_key, dims, shards, least, top_value):
    loudness, own = 1.0, jax.random.fold_in(stream_key, 6)
    for axis_at, parts in shards:
        draws = jnp.exp(jax.random.uniform(jax.random.fold_in(own, axis_at), (parts,), jnp.float32, least / len(shards), top_value / len(shards)))
        loudness = loudness * jnp.repeat(draws, dims[axis_at] // parts).reshape([-1 if axis == axis_at else 1 for axis in range(len(dims))])
    return loudness


def gaussian(rng, extent, width, limit, cuts=(), dtype=jnp.bfloat16):
    array = width * jax.random.normal(rng, extent, jnp.float32)
    if cuts:
        array = array * steps_of(rng, extent, cuts, -0.22, 0.18)
    return jnp.clip(array, -limit, limit).astype(dtype)


def setup_inputs(seed: int = 0, part: int = 0) -> dict:
    seeds = jax.random.split(jax.random.key(seed), 8)
    own_keys = jax.random.split(jax.random.fold_in(seeds[7], part), 8)
    queries = draw_queries(jax.random.fold_in(jax.random.fold_in(seeds[7], part), 71), part)
    latent_pages = draw_latent_pages(jax.random.fold_in(jax.random.fold_in(seeds[7], part), 71), part)
    page_scales = jnp.clip(jnp.exp(math.log(2.0) - 1.3862944 * jax.random.uniform(own_keys[2], (REQS, PAGES_REQ, GROUPS, PAGE), jnp.float32) ** steps_of(own_keys[2], (REQS, PAGES_REQ, GROUPS, PAGE), ((0, 8), (1, 2)), -0.2, 0.2)), 0.5, 2.0).astype(jnp.bfloat16)
    page_table = jax.vmap(lambda own: jax.random.permutation(own, PAGES_REQ))(jax.random.split(own_keys[3], REQS)).reshape((REQS, PAGES_REQ)).astype(jnp.int32)
    lengths = draw_lengths(jax.random.fold_in(jax.random.fold_in(seeds[7], part), 71), part)
    w_keys = gaussian(seeds[5], (LATENT, HEADS, NOPE), (LATENT // 4) ** -0.5, 0.5, ((0, 8), (1, 2)))
    w_values = gaussian(seeds[6], (LATENT, HEADS, VDIM), (LATENT // 16) ** -0.5, 1.0, ((0, 8), (1, 2)))
    return {"queries": queries, "latent_pages": latent_pages, "page_scales": page_scales, "page_table": page_table, "lengths": lengths, "w_keys": w_keys, "w_values": w_values}


def one_request(span_query, pool_pages, pool_scales, pool_table, length_one, w_keys, w_values):
    ordered = jnp.take(pool_pages, pool_table.astype(jnp.int32), axis=0)
    ordered_scales = jnp.take(pool_scales, pool_table.astype(jnp.int32), axis=0)
    key_count = PAGES_REQ * PAGE
    code_values = ordered[:, :, :LATENT].astype(jnp.float32).reshape(PAGES_REQ, PAGE, GROUPS, LATENT // GROUPS)
    factor = jnp.swapaxes(ordered_scales, 1, 2).astype(jnp.float32)[..., None]
    latent = (code_values * factor).reshape(key_count, LATENT).astype(jnp.bfloat16)
    rotary = ordered[:, :, LATENT:].reshape(key_count, ROPE)
    key_nope = jnp.dot(latent, w_keys.reshape(LATENT, HEADS * NOPE), preferred_element_type=jnp.float32)
    key_nope = key_nope.astype(jnp.bfloat16).reshape(key_count, HEADS, NOPE)
    value_rows = jnp.dot(latent, w_values.reshape(LATENT, HEADS * VDIM), preferred_element_type=jnp.float32)
    value_rows = value_rows.astype(jnp.bfloat16).reshape(key_count, HEADS, VDIM)
    query_nope = span_query[:, :, :NOPE].astype(jnp.float32)
    query_rope = span_query[:, :, NOPE:].astype(jnp.float32)
    scores = jnp.einsum('chn,khn->hck', query_nope, key_nope.astype(jnp.float32))
    scores = scores + jnp.einsum('chr,kr->hck', query_rope, rotary.astype(jnp.float32))
    scores = scores * (1.0 / math.sqrt(NOPE + ROPE))
    row_position = lax.broadcasted_iota(jnp.int32, (SPAN, key_count), 0)
    key_position = lax.broadcasted_iota(jnp.int32, (SPAN, key_count), 1)
    visible = (key_position <= length_one.astype(jnp.int32) - SPAN + row_position)[None]
    row_top = lax.optimization_barrier(jnp.max(jnp.where(visible, scores, -jnp.inf), axis=2))
    raw_weight = jnp.where(visible, jnp.exp(scores - row_top[..., None]), 0.0)
    row_total = lax.optimization_barrier(jnp.sum(raw_weight, axis=2))
    weights = raw_weight.astype(jnp.bfloat16)
    summed = jnp.einsum('hck,khv->chv', weights.astype(jnp.float32), value_rows.astype(jnp.float32))
    return (summed / jnp.swapaxes(row_total, 0, 1)[..., None]).astype(jnp.bfloat16)

def reference(queries, latent_pages, page_scales, page_table, lengths, w_keys, w_values):

    def handle(operands):
        return one_request(operands[0], operands[1], operands[2], operands[3], operands[4], w_keys, w_values)
    return lax.map(handle, (queries, latent_pages, page_scales, page_table, lengths))
```

```python
import functools
import math

import jax
import jax.numpy as jnp
from jax import lax
from jax.experimental import pallas as pl
from jax.experimental.pallas import tpu as pltpu
from jax.sharding import PartitionSpec as P

NEGATIVE = -1e30
MESH = pl.DeviceIdType.MESH
PAIR = 2
LAG = 2
AHEAD = 2


def attend_block(
    running, span_query, page_data, page_factor, first_key, row_offset, up_keys, up_values
):
    row_top, row_total, summed = running
    latent_width = up_keys.shape[0]
    group_count = page_factor.shape[1]
    page_rows = page_data.shape[1]
    key_count = page_data.shape[0] * page_rows
    head_count = span_query.shape[1]
    code_values = page_data[:, :, :latent_width].astype(jnp.float32)
    code_values = code_values.reshape(
        page_data.shape[0], page_rows, group_count, latent_width // group_count
    )
    factor = jnp.swapaxes(page_factor, 1, 2).astype(jnp.float32)[..., None]
    latent = (code_values * factor).reshape(key_count, latent_width).astype(jnp.bfloat16)
    rotary = page_data[:, :, latent_width:].reshape(key_count, -1)
    key_nope = jnp.dot(latent, up_keys, preferred_element_type=jnp.float32).astype(jnp.bfloat16)
    key_nope = key_nope.reshape(key_count, head_count, -1)
    value_rows = jnp.dot(latent, up_values, preferred_element_type=jnp.float32).astype(jnp.bfloat16)
    value_rows = value_rows.reshape(key_count, head_count, -1)
    nope_width = key_nope.shape[2]
    scores = jnp.einsum(
        "chn,khn->hck", span_query[:, :, :nope_width], key_nope, preferred_element_type=jnp.float32
    )
    scores = scores + jnp.einsum(
        "chr,kr->hck", span_query[:, :, nope_width:], rotary, preferred_element_type=jnp.float32
    )
    scores = scores * (1.0 / math.sqrt(span_query.shape[2]))
    row_position = lax.broadcasted_iota(jnp.int32, (span_query.shape[0], key_count), 0)
    key_position = first_key + lax.broadcasted_iota(jnp.int32, (span_query.shape[0], key_count), 1)
    visible = (key_position <= row_offset + row_position)[None]
    new_top = jnp.maximum(row_top, jnp.max(jnp.where(visible, scores, NEGATIVE), axis=2))
    raw_weight = jnp.where(visible, jnp.exp(scores - new_top[..., None]), 0.0)
    rescale = jnp.exp(row_top - new_top)
    row_total = row_total * rescale + jnp.sum(raw_weight, axis=2)
    weights = raw_weight.astype(jnp.bfloat16)
    summed = summed * jnp.swapaxes(rescale, 0, 1)[..., None] + jnp.einsum(
        "hck,khv->chv", weights, value_rows, preferred_element_type=jnp.float32
    )
    return (new_top, row_total, summed)


def sweep(span_query, row_offset, first_block, stop_block, fetch, up_keys, up_values):
    row_count = span_query.shape[0]
    head_count = span_query.shape[1]
    value_width = up_values.shape[1] // head_count
    initial = (
        jnp.full((head_count, row_count), NEGATIVE, jnp.float32),
        jnp.zeros((head_count, row_count), jnp.float32),
        jnp.zeros((row_count, head_count, value_width), jnp.float32),
    )

    def advance(block_index, running):
        page_data, page_factor, first_key = fetch(block_index)
        return attend_block(
            running, span_query, page_data, page_factor, first_key, row_offset, up_keys, up_values
        )

    return lax.fori_loop(first_block, stop_block, advance, initial)


def finish(row_total, summed):
    return (summed / jnp.swapaxes(row_total, 0, 1)[..., None]).astype(jnp.bfloat16)[None]


def on_device(queries, latent_pages, page_scales, page_table, lengths, w_keys, w_values):
    pool_pages, pool_scales = (
        lax.all_gather(latent_pages, "head", axis=1, tiled=True),
        lax.all_gather(page_scales, "head", axis=1, tiled=True),
    )
    full_keys, full_values = (
        lax.all_gather(w_keys, "ctx", axis=0, tiled=True),
        lax.all_gather(w_values, "ctx", axis=0, tiled=True),
    )
    latent_width = full_keys.shape[0]
    up_keys = full_keys.reshape(latent_width, -1)
    up_values = full_values.reshape(latent_width, -1)
    span_query = queries[0]
    own_pages = pool_pages[0]
    own_scales = pool_scales[0]
    own_table = page_table[0]
    row_count = span_query.shape[0]
    block_keys = 2 * own_pages.shape[1]
    own_length = lengths[0]
    block_count = (own_length + block_keys - 1) // block_keys

    def own_fetch(block_index):
        pool_slots = lax.dynamic_slice_in_dim(own_table, 2 * block_index, 2)
        return (
            jnp.take(own_pages, pool_slots, axis=0),
            jnp.take(own_scales, pool_slots, axis=0),
            block_index * block_keys,
        )

    row_top, row_total, summed = sweep(
        span_query, own_length - row_count, 0, block_count, own_fetch, up_keys, up_values
    )
    return finish(row_total, summed)


def gather_attend(
    shard_columns, q_in, pages_in, scales_in, table_in, wk_in, wv_in, length_in, out,
    q_rx, q_own, k_all, pages, scales, table, t_own, t_rx, wk_raw, wv_raw, w_all, rot, late,
    stage, own_sem, core_send, core_recv, relay_send, relay_recv, k_send, k_recv, t_send, t_recv,
    q_send, q_recv, z_send, z_recv, x_send, x_recv, f_send, f_recv,
    r_send, g_send, o_send, o_recv
):
    chunk_count = w_all.shape[0]
    latent_rows = w_all.shape[3]
    latent_width = w_all.shape[2] * latent_rows
    span = q_in.shape[-1]
    nope = w_all.shape[-1] // 2
    rope = q_in.shape[-2] - nope
    half_heads = chunk_count * PAIR
    page_count, page = k_all.shape[2], k_all.shape[3]
    key_count = 2 * page_count * page
    group_count = scales.shape[1]
    group_width = latent_width // group_count
    scale = 1.0 / math.sqrt(nope + rope)
    y, ctx, core = lax.axis_index("groups"), lax.axis_index("ctx"), lax.axis_index("head")
    row, side = ctx // 2, lax.rem(ctx, 2)
    last = shard_columns - 1
    y_peer = {"groups": 1 - y}
    core_peer = {"head": 1 - core}
    x_peer = {"ctx": 2 * row + 1 - side}
    partner = row + 1 - 2 * lax.rem(row, 2)

    def column(other):
        return {"ctx": 2 * other + side}

    def exists(other):
        return jnp.logical_and(other >= 0, other <= last)

    def local(source, target, index):
        return pltpu.make_async_copy(source, target, own_sem.at[index])

    heads_here = pl.ds(pl.multiple_of(y * half_heads, half_heads), half_heads)
    loads = [
        local(wk_in.at[:, heads_here], wk_raw, 0),
        local(wv_in.at[:, heads_here], wv_raw, 1),
        local(pages_in, pages, 2),
        local(scales_in, scales, 3),
        local(table_in, table, 4),
        local(q_in.at[y], q_own, 5),
    ]
    for load in loads:
        load.start()

    barrier = pltpu.get_barrier_semaphore()
    peers = [y_peer, core_peer, x_peer]
    peers += [column(lax.rem(row + d, shard_columns)) for d in range(1, shard_columns)]
    for peer in peers:
        pl.semaphore_signal(barrier, inc=1, device_id=peer, device_id_type=MESH)

    def remote(source, target, send, recv, peer):
        return pltpu.make_async_remote_copy(
            src_ref=source, dst_ref=target, send_sem=send, recv_sem=recv,
            device_id=peer, device_id_type=MESH,
        )

    def moved(c, source_row, source_side, send, recv, peer):
        block = w_all.at[c, :, 2 * source_row + source_side]
        return remote(block, block, send, recv, peer)

    k_mine = k_all.at[y, core]
    k_copy = remote(k_mine, k_mine, k_send, k_recv, y_peer)
    t_copy = remote(t_own, t_rx, t_send, t_recv, y_peer)
    core_copy = remote(k_mine, k_mine, core_send, core_recv, core_peer)
    k_other = k_all.at[1 - y, core]
    relay_copy = remote(k_other, k_other, relay_send, relay_recv, core_peer)

    def q_copy(c):
        return remote(q_in.at[1 - y, c], q_rx.at[c], q_send.at[c], q_recv.at[c], y_peer)

    hops = [(distance, step) for distance in (1, 2) for step in (1, -1)]

    def z_copy(c, index):
        distance, step = hops[index]
        return moved(
            c, row, side, z_send.at[c, index], z_recv.at[c, row], column(row + step * distance)
        )

    def z_arrival(c, source):
        return moved(c, source, side, z_send.at[c, 0], z_recv.at[c, source], x_peer)

    def r_copy(c, step):
        source = row + 2 * step
        return moved(c, source, side, r_send.at[c], z_recv.at[c, source], column(row - step))

    def x_copy(c):
        return moved(c, row, side, x_send.at[c], x_recv.at[c], x_peer)

    def x_arrival(c):
        return moved(c, row, 1 - side, x_send.at[c], x_recv.at[c], x_peer)

    def f_copy(c, source):
        return moved(c, source, side, f_send.at[c, source], f_recv.at[c, source], x_peer)

    def f_arrival(c, source):
        return moved(c, source, 1 - side, f_send.at[c, source], f_recv.at[c, source], x_peer)

    def g_copy(c):
        return moved(c, row, 1 - side, g_send.at[c], f_recv.at[c, row], column(partner))

    def by_z(c):
        return lax.rem(c, 2) == 1

    def over_x(c, source):
        return jnp.logical_or(jnp.logical_not(by_z(c)), source != partner)

    def o_copy(c):
        return remote(stage.at[c], out.at[y, c], o_send.at[c], o_recv.at[c], y_peer)

    def send_own(c):
        for index, (distance, step) in enumerate(hops):
            @pl.when(exists(row + step * distance))
            def _():
                z_copy(c, index).start()

        x_copy(c).start()

    loads[0].wait()
    loads[1].wait()
    keys_by_head = jnp.swapaxes(wk_raw[...], 0, 1)
    values_by_head = jnp.swapaxes(wv_raw[...], 0, 1)
    for c in range(chunk_count):
        for h in range(PAIR):
            w_all[c, h, ctx, :, :nope] = keys_by_head[c * PAIR + h]
            w_all[c, h, ctx, :, nope:] = values_by_head[c * PAIR + h]

    pl.semaphore_wait(barrier, len(peers))
    for c in range(AHEAD):
        send_own(c)

    loads[2].wait()
    loads[3].wait()
    columns = jnp.transpose(
        scales[...].astype(jnp.float32).reshape(page_count * group_count, page)
    )
    for p in range(page_count):
        for g in range(group_count):
            part = pl.ds(g * group_width, group_width)
            at = p * group_count + g
            codes = pages[p, :, part].astype(jnp.float32)
            k_all[y, core, p, :, part] = (codes * columns[:, at : at + 1]).astype(jnp.bfloat16)
        k_all[y, core, p, :, latent_width:] = pages[p, :, latent_width:]
    k_copy.start()
    core_copy.start()
    loads[4].wait()
    slots = 2 * page_count
    slot = lax.broadcasted_iota(jnp.int32, (slots, slots), 0)
    place = lax.broadcasted_iota(jnp.int32, (slots, slots), 1)
    order = jnp.sum(jnp.where(table[...] == slot, place, 0), axis=1, keepdims=True)
    t_own[...] = jnp.broadcast_to(order * page - (length_in[0] - span), t_own.shape)
    t_copy.start()

    def send_queries(c, carry):
        q_copy(c).start()
        return carry

    lax.fori_loop(0, chunk_count, send_queries, 0)
    loads[5].wait()

    def settle():
        t_copy.wait_recv()
        core_copy.wait_recv()
        relay_copy.wait_recv()
        offset = lax.broadcasted_iota(jnp.int32, (page, span), 0)
        offset = offset - lax.broadcasted_iota(jnp.int32, (page, span), 1)
        for request, t_ref in ((y, t_own), (1 - y, t_rx)):
            rot[request] = k_all[request, :, :, :, latent_width:].reshape(key_count, rope)
            late[request] = jnp.concatenate(
                [t_ref[p : p + 1] + offset for p in range(slots)], axis=0
            )

    def attend(c, h, request, q_ref):
        latent = k_all[request, :, :, :, :latent_width].reshape(key_count, latent_width)
        visible = late[request] <= 0
        weight = w_all[c, h].reshape(latent_width, -1)
        up = jnp.dot(latent, weight, preferred_element_type=jnp.float32).astype(jnp.bfloat16)
        keys = jnp.concatenate([up[:, :nope], rot[request]], axis=1)
        scores = jnp.dot(keys, q_ref[c, h], preferred_element_type=jnp.float32)
        scores = jnp.where(visible, scores * scale, NEGATIVE)
        top = jnp.max(scores, axis=0, keepdims=True)
        raw = jnp.where(visible, jnp.exp(scores - top), 0.0)
        total = jnp.sum(raw, axis=0, keepdims=True)
        summed = lax.dot_general(
            up[:, nope:], raw.astype(jnp.bfloat16), (((0,), (0,)), ((), ())),
            preferred_element_type=jnp.float32,
        )
        return jnp.transpose(summed / total).astype(jnp.bfloat16)

    def pass_on(c, distance):
        for step in (1, -1):
            source = row + step * distance

            @pl.when(exists(source))
            def _():
                z_arrival(c, source).wait_recv()
                if distance == 2:
                    @pl.when(exists(row - step))
                    def _():
                        r_copy(c, step).start()

                @pl.when(over_x(c, source))
                def _():
                    f_copy(c, source).start()

    def advance(c, carry):
        @pl.when(c + AHEAD < chunk_count)
        def _():
            send_own(c + AHEAD)

        sending = c < chunk_count
        ready = c >= LAG
        b = jnp.maximum(c - LAG, 0)
        for unit in range(2 * PAIR):
            if unit == 0:
                @pl.when(sending)
                def _():
                    pass_on(c, 1)
                    x_arrival(c).wait_recv()

                    @pl.when(by_z(c))
                    def _():
                        g_copy(c).start()
            elif unit < shard_columns - 1:
                @pl.when(sending)
                def _():
                    pass_on(c, unit + 1)

            if unit == shard_columns - 2:
                @pl.when(c == 1)
                def _():
                    k_copy.wait_recv()
                    relay_copy.start()

            if unit == 0:
                @pl.when(c == LAG)
                def _():
                    settle()

            @pl.when(ready)
            def _():
                if unit == 0:
                    for d in range(1, shard_columns):
                        f_arrival(b, lax.rem(row + d, shard_columns)).wait_recv()
                    q_copy(b).wait_recv()
                h = unit % PAIR
                if unit < PAIR:
                    stage[b, h] = attend(b, h, 1 - y, q_rx)
                    if unit == PAIR - 1:
                        o_copy(b).start()
                else:
                    out[y, b, h] = attend(b, h, y, q_own)

        return carry

    lax.fori_loop(0, chunk_count + LAG, advance, 0)
    k_copy.wait_send()
    t_copy.wait_send()
    core_copy.wait_send()
    relay_copy.wait_send()

    def end(c, carry):
        q_copy(c).wait_send()
        x_copy(c).wait_send()
        for index, (distance, step) in enumerate(hops):
            @pl.when(exists(row + step * distance))
            def _():
                z_copy(c, index).wait_send()

            if distance == 2:
                @pl.when(jnp.logical_and(exists(row + 2 * step), exists(row - step)))
                def _():
                    r_copy(c, step).wait_send()

        for d in range(1, shard_columns):
            other = lax.rem(row + d, shard_columns)

            @pl.when(over_x(c, other))
            def _():
                f_copy(c, other).wait_send()

        @pl.when(by_z(c))
        def _():
            g_copy(c).wait_send()

        return carry

    lax.fori_loop(0, chunk_count, end, 0)

    def end_out(c, carry):
        o_copy(c).wait()
        return carry

    lax.fori_loop(0, chunk_count, end_out, 0)


def shared_on_device(
    shards, queries, latent_pages, page_scales, page_table, lengths, w_keys, w_values
):
    _, span, heads, _ = queries.shape
    latent_rows, _, nope = w_keys.shape
    _, slots, page, width = latent_pages.shape
    latent_width = latent_rows * shards
    rope = width - latent_width
    groups = page_scales.shape[2]
    chunks = heads // (2 * PAIR)
    pool = page_table.shape[1]
    columns = shards // 2
    half = heads // 2
    q_in = jnp.transpose(queries[0], (1, 2, 0)).reshape(2, chunks, PAIR, -1, span)
    operands = (
        q_in, latent_pages[0], page_scales[0], page_table, w_keys, w_values
    )
    dma, vmem = pltpu.SemaphoreType.DMA, pltpu.VMEM
    bf16, int32 = jnp.bfloat16, jnp.int32
    out = pl.pallas_call(
        functools.partial(gather_attend, columns),
        out_shape=vmem((2, chunks, PAIR, span, nope), bf16),
        in_specs=[pl.BlockSpec(memory_space=pltpu.HBM)] * 6
        + [pl.BlockSpec(memory_space=pltpu.SMEM)],
        out_specs=pl.BlockSpec(memory_space=vmem),
        scratch_shapes=[
            vmem(q_in.shape[1:], bf16),
            vmem(q_in.shape[1:], bf16),
            vmem((2, 2, slots, page, width), bf16),
            vmem((slots, page, width), bf16),
            vmem((slots, groups, page), bf16),
            vmem((1, pool), int32),
            vmem((pool, span), int32),
            vmem((pool, span), int32),
            vmem((latent_rows, half, nope), bf16),
            vmem((latent_rows, half, nope), bf16),
            vmem((chunks, PAIR, shards, latent_rows, 2 * nope), bf16),
            vmem((2, pool * page, rope), bf16),
            vmem((2, pool * page, span), int32),
            vmem((chunks, PAIR, span, nope), bf16),
            dma((6,)), dma, dma, dma, dma, dma, dma, dma, dma,
            dma((chunks,)), dma((chunks,)),
            dma((chunks, 4)), dma((chunks, columns)),
            dma((chunks,)), dma((chunks,)),
            dma((chunks, columns)), dma((chunks, columns)),
            dma((chunks,)), dma((chunks,)), dma((chunks,)), dma((chunks,)),
        ],
        compiler_params=pltpu.CompilerParams(
            collective_id=0, has_side_effects=True, vmem_limit_bytes=48 * 1024 * 1024
        ),
    )(*(pltpu.with_memory_space_constraint(x, pltpu.HBM) for x in operands), lengths)
    return jnp.swapaxes(out.reshape(heads, span, nope), 0, 1)[None]


def body_for(mesh, queries, latent_pages, page_scales, page_table, lengths, w_keys, w_values):
    args = (queries, latent_pages, page_scales, page_table, lengths, w_keys, w_values)
    shards = mesh.shape["ctx"]
    rope = latent_pages.shape[3] - w_keys.shape[0] * shards
    fits = (
        mesh.shape["groups"] == 2 and mesh.shape["head"] == 2 and shards == 8
        and w_keys.shape[0] % 16 == 0 and queries.shape[2] % 16 == 0
        and w_keys.shape == w_values.shape and 2 * rope == w_keys.shape[2]
    )
    if fits:
        return shared_on_device(shards, *args)
    return on_device(*args)


def solution(mesh):
    return jax.shard_map(
        functools.partial(body_for, mesh),
        mesh=mesh,
        in_specs=(
            P(("groups", "ctx"), None, "head", None),
            P(("groups", "ctx"), "head", None, None),
            P(("groups", "ctx"), "head", None, None),
            P(("groups", "ctx"), None),
            P(("groups", "ctx")),
            P("ctx", "head", None),
            P("ctx", "head", None),
        ),
        out_specs=P(("groups", "ctx"), None, "head", None),
        check_vma=False,
    )
```

```python
import functools
import math

import jax
import jax.numpy as jnp
from jax import lax
from jax.experimental import pallas as pl
from jax.experimental.pallas import tpu as pltpu
from jax.sharding import PartitionSpec as P

NEGATIVE = -1e30
MESH = pl.DeviceIdType.MESH
PAIR = 2
LAG = 2
AHEAD = 3


def attend_block(
    running, span_query, page_data, page_factor, first_key, row_offset, up_keys, up_values
):
    row_top, row_total, summed = running
    latent_width = up_keys.shape[0]
    group_count = page_factor.shape[1]
    page_rows = page_data.shape[1]
    key_count = page_data.shape[0] * page_rows
    head_count = span_query.shape[1]
    code_values = page_data[:, :, :latent_width].astype(jnp.float32)
    code_values = code_values.reshape(
        page_data.shape[0], page_rows, group_count, latent_width // group_count
    )
    factor = jnp.swapaxes(page_factor, 1, 2).astype(jnp.float32)[..., None]
    latent = (code_values * factor).reshape(key_count, latent_width).astype(jnp.bfloat16)
    rotary = page_data[:, :, latent_width:].reshape(key_count, -1)
    key_nope = jnp.dot(latent, up_keys, preferred_element_type=jnp.float32).astype(jnp.bfloat16)
    key_nope = key_nope.reshape(key_count, head_count, -1)
    value_rows = jnp.dot(latent, up_values, preferred_element_type=jnp.float32).astype(jnp.bfloat16)
    value_rows = value_rows.reshape(key_count, head_count, -1)
    nope_width = key_nope.shape[2]
    scores = jnp.einsum(
        "chn,khn->hck", span_query[:, :, :nope_width], key_nope, preferred_element_type=jnp.float32
    )
    scores = scores + jnp.einsum(
        "chr,kr->hck", span_query[:, :, nope_width:], rotary, preferred_element_type=jnp.float32
    )
    scores = scores * (1.0 / math.sqrt(span_query.shape[2]))
    row_position = lax.broadcasted_iota(jnp.int32, (span_query.shape[0], key_count), 0)
    key_position = first_key + lax.broadcasted_iota(jnp.int32, (span_query.shape[0], key_count), 1)
    visible = (key_position <= row_offset + row_position)[None]
    new_top = jnp.maximum(row_top, jnp.max(jnp.where(visible, scores, NEGATIVE), axis=2))
    raw_weight = jnp.where(visible, jnp.exp(scores - new_top[..., None]), 0.0)
    rescale = jnp.exp(row_top - new_top)
    row_total = row_total * rescale + jnp.sum(raw_weight, axis=2)
    weights = raw_weight.astype(jnp.bfloat16)
    summed = summed * jnp.swapaxes(rescale, 0, 1)[..., None] + jnp.einsum(
        "hck,khv->chv", weights, value_rows, preferred_element_type=jnp.float32
    )
    return (new_top, row_total, summed)


def sweep(span_query, row_offset, first_block, stop_block, fetch, up_keys, up_values):
    row_count = span_query.shape[0]
    head_count = span_query.shape[1]
    value_width = up_values.shape[1] // head_count
    initial = (
        jnp.full((head_count, row_count), NEGATIVE, jnp.float32),
        jnp.zeros((head_count, row_count), jnp.float32),
        jnp.zeros((row_count, head_count, value_width), jnp.float32),
    )

    def advance(block_index, running):
        page_data, page_factor, first_key = fetch(block_index)
        return attend_block(
            running, span_query, page_data, page_factor, first_key, row_offset, up_keys, up_values
        )

    return lax.fori_loop(first_block, stop_block, advance, initial)


def finish(row_total, summed):
    return (summed / jnp.swapaxes(row_total, 0, 1)[..., None]).astype(jnp.bfloat16)[None]


def on_device(queries, latent_pages, page_scales, page_table, lengths, w_keys, w_values):
    pool_pages, pool_scales = (
        lax.all_gather(latent_pages, "head", axis=1, tiled=True),
        lax.all_gather(page_scales, "head", axis=1, tiled=True),
    )
    full_keys, full_values = (
        lax.all_gather(w_keys, "ctx", axis=0, tiled=True),
        lax.all_gather(w_values, "ctx", axis=0, tiled=True),
    )
    latent_width = full_keys.shape[0]
    up_keys = full_keys.reshape(latent_width, -1)
    up_values = full_values.reshape(latent_width, -1)
    span_query = queries[0]
    own_pages = pool_pages[0]
    own_scales = pool_scales[0]
    own_table = page_table[0]
    row_count = span_query.shape[0]
    block_keys = 2 * own_pages.shape[1]
    own_length = lengths[0]
    block_count = (own_length + block_keys - 1) // block_keys

    def own_fetch(block_index):
        pool_slots = lax.dynamic_slice_in_dim(own_table, 2 * block_index, 2)
        return (
            jnp.take(own_pages, pool_slots, axis=0),
            jnp.take(own_scales, pool_slots, axis=0),
            block_index * block_keys,
        )

    row_top, row_total, summed = sweep(
        span_query, own_length - row_count, 0, block_count, own_fetch, up_keys, up_values
    )
    return finish(row_total, summed)


def gather_attend(
    shard_columns, q_in, pages_in, scales_in, table_in, wk_in, wv_in, length_in, out,
    q_rx, q_own, k_all, pages, scales, table, t_own, t_rx, wk_raw, wv_raw, w_all, rot, late,
    stage, own_sem, core_send, core_recv, relay_send, relay_recv, k_send, k_recv, t_send, t_recv,
    q_send, q_recv, z_send, z_recv, x_send, x_recv, f_send, f_recv,
    r_send, g_send, o_send, o_recv
):
    chunk_count = w_all.shape[0]
    latent_rows = w_all.shape[3]
    latent_width = w_all.shape[2] * latent_rows
    span = q_in.shape[-1]
    nope = w_all.shape[-1] // 2
    rope = q_in.shape[-2] - nope
    half_heads = chunk_count * PAIR
    page_count, page = k_all.shape[2], k_all.shape[3]
    key_count = 2 * page_count * page
    group_count = scales.shape[1]
    group_width = latent_width // group_count
    scale = 1.0 / math.sqrt(nope + rope)
    y, ctx, core = lax.axis_index("groups"), lax.axis_index("ctx"), lax.axis_index("head")
    row, side = ctx // 2, lax.rem(ctx, 2)
    last = shard_columns - 1
    y_peer = {"groups": 1 - y}
    core_peer = {"head": 1 - core}
    x_peer = {"ctx": 2 * row + 1 - side}
    partner = row + 1 - 2 * lax.rem(row, 2)

    def column(other):
        return {"ctx": 2 * other + side}

    def exists(other):
        return jnp.logical_and(other >= 0, other <= last)

    def local(source, target, index):
        return pltpu.make_async_copy(source, target, own_sem.at[index])

    heads_here = pl.ds(pl.multiple_of(y * half_heads, half_heads), half_heads)
    loads = [
        local(wk_in.at[:, heads_here], wk_raw, 0),
        local(wv_in.at[:, heads_here], wv_raw, 1),
        local(pages_in, pages, 2),
        local(scales_in, scales, 3),
        local(table_in, table, 4),
        local(q_in.at[y], q_own, 5),
    ]
    for load in loads:
        load.start()

    barrier = pltpu.get_barrier_semaphore()
    peers = [y_peer, core_peer, x_peer]
    peers += [column(lax.rem(row + d, shard_columns)) for d in range(1, shard_columns)]
    for peer in peers:
        pl.semaphore_signal(barrier, inc=1, device_id=peer, device_id_type=MESH)

    def remote(source, target, send, recv, peer):
        return pltpu.make_async_remote_copy(
            src_ref=source, dst_ref=target, send_sem=send, recv_sem=recv,
            device_id=peer, device_id_type=MESH,
        )

    def moved(c, source_row, source_side, send, recv, peer):
        block = w_all.at[c, :, 2 * source_row + source_side]
        return remote(block, block, send, recv, peer)

    k_mine = k_all.at[y, core]
    k_copy = remote(k_mine, k_mine, k_send, k_recv, y_peer)
    t_copy = remote(t_own, t_rx, t_send, t_recv, y_peer)
    core_copy = remote(k_mine, k_mine, core_send, core_recv, core_peer)
    k_other = k_all.at[1 - y, core]
    relay_copy = remote(k_other, k_other, relay_send, relay_recv, core_peer)

    def q_copy(c):
        return remote(q_in.at[1 - y, c], q_rx.at[c], q_send, q_recv.at[c], y_peer)

    hops = [(distance, step) for distance in (1, 2) for step in (1, -1)]

    def z_copy(c, index):
        distance, step = hops[index]
        return moved(
            c, row, side, z_send.at[index], z_recv.at[c, row], column(row + step * distance)
        )

    def z_arrival(c, source):
        return moved(c, source, side, z_send.at[0], z_recv.at[c, source], x_peer)

    def r_copy(c, step):
        source = row + 2 * step
        return moved(c, source, side, r_send, z_recv.at[c, source], column(row - step))

    def x_copy(c):
        return moved(c, row, side, x_send, x_recv.at[c], x_peer)

    def x_arrival(c):
        return moved(c, row, 1 - side, x_send, x_recv.at[c], x_peer)

    def f_copy(c, source):
        return moved(c, source, side, f_send.at[source], f_recv.at[c], x_peer)

    def f_arrivals(c):
        blocks = w_all.at[c, :, 0:last]
        return remote(blocks, blocks, x_send, f_recv.at[c], x_peer)

    def sent(count, semaphore):
        blocks = w_all.at[0:count, :, 0]
        return remote(blocks, blocks, semaphore, x_recv.at[0], x_peer)

    def g_copy(c):
        return moved(c, row, 1 - side, g_send, f_recv.at[c], column(partner))

    def by_z(c):
        return c >= chunk_count // 2

    def over_x(c, source):
        return jnp.logical_or(jnp.logical_not(by_z(c)), source != partner)

    def o_copy(c):
        return remote(stage.at[c], out.at[y, c], o_send, o_recv, y_peer)

    def send_own(c):
        for index, (distance, step) in enumerate(hops):
            @pl.when(exists(row + step * distance))
            def _():
                z_copy(c, index).start()

        x_copy(c).start()

    loads[0].wait()
    loads[1].wait()
    keys_by_head = jnp.swapaxes(wk_raw[...], 0, 1)
    values_by_head = jnp.swapaxes(wv_raw[...], 0, 1)
    for c in range(chunk_count):
        for h in range(PAIR):
            w_all[c, h, ctx, :, :nope] = keys_by_head[c * PAIR + h]
            w_all[c, h, ctx, :, nope:] = values_by_head[c * PAIR + h]

    pl.semaphore_wait(barrier, len(peers))
    for c in range(AHEAD):
        send_own(c)

    loads[2].wait()
    loads[3].wait()
    columns = jnp.transpose(
        scales[...].astype(jnp.float32).reshape(page_count * group_count, page)
    )
    for p in range(page_count):
        for g in range(group_count):
            part = pl.ds(g * group_width, group_width)
            at = p * group_count + g
            codes = pages[p, :, part].astype(jnp.float32)
            k_all[y, core, p, :, part] = (codes * columns[:, at : at + 1]).astype(jnp.bfloat16)
        k_all[y, core, p, :, latent_width:] = pages[p, :, latent_width:]
    k_copy.start()
    core_copy.start()
    loads[4].wait()
    slots = 2 * page_count
    slot = lax.broadcasted_iota(jnp.int32, (slots, slots), 0)
    place = lax.broadcasted_iota(jnp.int32, (slots, slots), 1)
    order = jnp.sum(jnp.where(table[...] == slot, place, 0), axis=1, keepdims=True)
    t_own[...] = jnp.broadcast_to(order * page - (length_in[0] - span), t_own.shape)
    t_copy.start()

    def send_queries(c, carry):
        q_copy(c).start()
        return carry

    lax.fori_loop(0, chunk_count, send_queries, 0)
    loads[5].wait()

    def settle():
        t_copy.wait_recv()
        core_copy.wait_recv()
        relay_copy.wait_recv()
        offset = lax.broadcasted_iota(jnp.int32, (page, span), 0)
        offset = offset - lax.broadcasted_iota(jnp.int32, (page, span), 1)
        for request, t_ref in ((y, t_own), (1 - y, t_rx)):
            rot[request] = k_all[request, :, :, :, latent_width:].reshape(key_count, rope)
            late[request] = jnp.concatenate(
                [t_ref[p : p + 1] + offset for p in range(slots)], axis=0
            )

    def attend(c, h, request, q_ref):
        latent = k_all[request, :, :, :, :latent_width].reshape(key_count, latent_width)
        visible = late[request] <= 0
        weight = w_all[c, h].reshape(latent_width, -1)
        up = jnp.dot(latent, weight, preferred_element_type=jnp.float32).astype(jnp.bfloat16)
        keys = jnp.concatenate([up[:, :nope], rot[request]], axis=1)
        scores = jnp.dot(keys, q_ref[c, h], preferred_element_type=jnp.float32)
        scores = jnp.where(visible, scores * scale, NEGATIVE)
        top = jnp.max(scores, axis=0, keepdims=True)
        raw = jnp.where(visible, jnp.exp(scores - top), 0.0)
        total = jnp.sum(raw, axis=0, keepdims=True)
        summed = lax.dot_general(
            up[:, nope:], raw.astype(jnp.bfloat16), (((0,), (0,)), ((), ())),
            preferred_element_type=jnp.float32,
        )
        return jnp.transpose(summed / total).astype(jnp.bfloat16)

    def pass_on(c, distance):
        for step in (1, -1):
            source = row + step * distance

            @pl.when(exists(source))
            def _():
                z_arrival(c, source).wait_recv()
                if distance == 2:
                    @pl.when(exists(row - step))
                    def _():
                        r_copy(c, step).start()

                @pl.when(over_x(c, source))
                def _():
                    f_copy(c, source).start()

    def advance(c, carry):
        @pl.when(c + AHEAD < chunk_count)
        def _():
            send_own(c + AHEAD)

        sending = c < chunk_count
        ready = c >= LAG
        b = jnp.maximum(c - LAG, 0)
        for unit in range(2 * PAIR):
            if unit == 0:
                @pl.when(sending)
                def _():
                    pass_on(c, 1)
            elif unit < shard_columns - 1:
                @pl.when(sending)
                def _():
                    pass_on(c, unit + 1)
                    if unit == shard_columns - 2:
                        x_arrival(c).wait_recv()

                        @pl.when(by_z(c))
                        def _():
                            g_copy(c).start()

            if unit == shard_columns - 2:
                @pl.when(c == 1)
                def _():
                    k_copy.wait_recv()
                    relay_copy.start()

            if unit == 0:
                @pl.when(c == LAG)
                def _():
                    settle()

            @pl.when(ready)
            def _():
                if unit == 0:
                    f_arrivals(b).wait_recv()
                    q_copy(b).wait_recv()
                h = unit % PAIR
                if unit < PAIR:
                    stage[b, h] = attend(b, h, 1 - y, q_rx)
                    if unit == PAIR - 1:
                        o_copy(b).start()
                else:
                    out[y, b, h] = attend(b, h, y, q_own)

        return carry

    lax.fori_loop(0, chunk_count + LAG, advance, 0)
    k_copy.wait_send()
    t_copy.wait_send()
    core_copy.wait_send()
    relay_copy.wait_send()

    direct = chunk_count // 2
    q_all = q_in.at[1 - y]
    remote(q_all, q_all, q_send, q_recv.at[0], y_peer).wait_send()
    sent(chunk_count, x_send).wait_send()
    sent(direct, g_send).wait_send()
    for index, (distance, step) in enumerate(hops):
        @pl.when(exists(row + step * distance))
        def _():
            sent(chunk_count, z_send.at[index]).wait_send()

        if distance == 2:
            @pl.when(jnp.logical_and(exists(row + 2 * step), exists(row - step)))
            def _():
                sent(chunk_count, r_send).wait_send()

    for d in range(1, shard_columns):
        other = lax.rem(row + d, shard_columns)

        @pl.when(other == partner)
        def _():
            sent(chunk_count - direct, f_send.at[other]).wait_send()

        @pl.when(other != partner)
        def _():
            sent(chunk_count, f_send.at[other]).wait_send()

    remote(stage, out.at[y], o_send, o_recv, y_peer).wait()


def shared_on_device(
    shards, queries, latent_pages, page_scales, page_table, lengths, w_keys, w_values
):
    _, span, heads, _ = queries.shape
    latent_rows, _, nope = w_keys.shape
    _, slots, page, width = latent_pages.shape
    latent_width = latent_rows * shards
    rope = width - latent_width
    groups = page_scales.shape[2]
    chunks = heads // (2 * PAIR)
    pool = page_table.shape[1]
    columns = shards // 2
    half = heads // 2
    q_in = jnp.transpose(queries[0], (1, 2, 0)).reshape(2, chunks, PAIR, -1, span)
    operands = (
        q_in, latent_pages[0], page_scales[0], page_table, w_keys, w_values
    )
    dma, vmem = pltpu.SemaphoreType.DMA, pltpu.VMEM
    bf16, int32 = jnp.bfloat16, jnp.int32
    out = pl.pallas_call(
        functools.partial(gather_attend, columns),
        out_shape=vmem((2, chunks, PAIR, span, nope), bf16),
        in_specs=[pl.BlockSpec(memory_space=pltpu.HBM)] * 6
        + [pl.BlockSpec(memory_space=pltpu.SMEM)],
        out_specs=pl.BlockSpec(memory_space=vmem),
        scratch_shapes=[
            vmem(q_in.shape[1:], bf16),
            vmem(q_in.shape[1:], bf16),
            vmem((2, 2, slots, page, width), bf16),
            vmem((slots, page, width), bf16),
            vmem((slots, groups, page), bf16),
            vmem((1, pool), int32),
            vmem((pool, span), int32),
            vmem((pool, span), int32),
            vmem((latent_rows, half, nope), bf16),
            vmem((latent_rows, half, nope), bf16),
            vmem((chunks, PAIR, shards, latent_rows, 2 * nope), bf16),
            vmem((2, pool * page, rope), bf16),
            vmem((2, pool * page, span), int32),
            vmem((chunks, PAIR, span, nope), bf16),
            dma((6,)), dma, dma, dma, dma, dma, dma, dma, dma,
            dma, dma((chunks,)),
            dma((4,)), dma((chunks, columns)),
            dma, dma((chunks,)),
            dma((columns,)), dma((chunks,)),
            dma, dma, dma, dma,
        ],
        compiler_params=pltpu.CompilerParams(
            collective_id=0, has_side_effects=True, vmem_limit_bytes=48 * 1024 * 1024
        ),
    )(*(pltpu.with_memory_space_constraint(x, pltpu.HBM) for x in operands), lengths)
    return jnp.swapaxes(out.reshape(heads, span, nope), 0, 1)[None]


def body_for(mesh, queries, latent_pages, page_scales, page_table, lengths, w_keys, w_values):
    args = (queries, latent_pages, page_scales, page_table, lengths, w_keys, w_values)
    shards = mesh.shape["ctx"]
    rope = latent_pages.shape[3] - w_keys.shape[0] * shards
    fits = (
        mesh.shape["groups"] == 2 and mesh.shape["head"] == 2 and shards == 8
        and w_keys.shape[0] % 16 == 0 and queries.shape[2] % 16 == 0
        and w_keys.shape == w_values.shape and 2 * rope == w_keys.shape[2]
    )
    if fits:
        return shared_on_device(shards, *args)
    return on_device(*args)


def solution(mesh):
    return jax.shard_map(
        functools.partial(body_for, mesh),
        mesh=mesh,
        in_specs=(
            P(("groups", "ctx"), None, "head", None),
            P(("groups", "ctx"), "head", None, None),
            P(("groups", "ctx"), "head", None, None),
            P(("groups", "ctx"), None),
            P(("groups", "ctx")),
            P("ctx", "head", None),
            P("ctx", "head", None),
        ),
        out_specs=P(("groups", "ctx"), None, "head", None),
        check_vma=False,
    )
```

```python
import functools
import math

import jax
import jax.numpy as jnp
from jax import lax
from jax.experimental import pallas as pl
from jax.experimental.pallas import tpu as pltpu
from jax.sharding import PartitionSpec as P

NEGATIVE = -1e30
MESH = pl.DeviceIdType.MESH
PAIR = 2
LAG = 2
AHEAD = 3


def attend_block(
    running, span_query, page_data, page_factor, first_key, row_offset, up_keys, up_values
):
    row_top, row_total, summed = running
    latent_width = up_keys.shape[0]
    group_count = page_factor.shape[1]
    page_rows = page_data.shape[1]
    key_count = page_data.shape[0] * page_rows
    head_count = span_query.shape[1]
    code_values = page_data[:, :, :latent_width].astype(jnp.float32)
    code_values = code_values.reshape(
        page_data.shape[0], page_rows, group_count, latent_width // group_count
    )
    factor = jnp.swapaxes(page_factor, 1, 2).astype(jnp.float32)[..., None]
    latent = (code_values * factor).reshape(key_count, latent_width).astype(jnp.bfloat16)
    rotary = page_data[:, :, latent_width:].reshape(key_count, -1)
    key_nope = jnp.dot(latent, up_keys, preferred_element_type=jnp.float32).astype(jnp.bfloat16)
    key_nope = key_nope.reshape(key_count, head_count, -1)
    value_rows = jnp.dot(latent, up_values, preferred_element_type=jnp.float32).astype(jnp.bfloat16)
    value_rows = value_rows.reshape(key_count, head_count, -1)
    nope_width = key_nope.shape[2]
    scores = jnp.einsum(
        "chn,khn->hck", span_query[:, :, :nope_width], key_nope, preferred_element_type=jnp.float32
    )
    scores = scores + jnp.einsum(
        "chr,kr->hck", span_query[:, :, nope_width:], rotary, preferred_element_type=jnp.float32
    )
    scores = scores * (1.0 / math.sqrt(span_query.shape[2]))
    row_position = lax.broadcasted_iota(jnp.int32, (span_query.shape[0], key_count), 0)
    key_position = first_key + lax.broadcasted_iota(jnp.int32, (span_query.shape[0], key_count), 1)
    visible = (key_position <= row_offset + row_position)[None]
    new_top = jnp.maximum(row_top, jnp.max(jnp.where(visible, scores, NEGATIVE), axis=2))
    raw_weight = jnp.where(visible, jnp.exp(scores - new_top[..., None]), 0.0)
    rescale = jnp.exp(row_top - new_top)
    row_total = row_total * rescale + jnp.sum(raw_weight, axis=2)
    weights = raw_weight.astype(jnp.bfloat16)
    summed = summed * jnp.swapaxes(rescale, 0, 1)[..., None] + jnp.einsum(
        "hck,khv->chv", weights, value_rows, preferred_element_type=jnp.float32
    )
    return (new_top, row_total, summed)


def sweep(span_query, row_offset, first_block, stop_block, fetch, up_keys, up_values):
    row_count = span_query.shape[0]
    head_count = span_query.shape[1]
    value_width = up_values.shape[1] // head_count
    initial = (
        jnp.full((head_count, row_count), NEGATIVE, jnp.float32),
        jnp.zeros((head_count, row_count), jnp.float32),
        jnp.zeros((row_count, head_count, value_width), jnp.float32),
    )

    def advance(block_index, running):
        page_data, page_factor, first_key = fetch(block_index)
        return attend_block(
            running, span_query, page_data, page_factor, first_key, row_offset, up_keys, up_values
        )

    return lax.fori_loop(first_block, stop_block, advance, initial)


def finish(row_total, summed):
    return (summed / jnp.swapaxes(row_total, 0, 1)[..., None]).astype(jnp.bfloat16)[None]


def on_device(queries, latent_pages, page_scales, page_table, lengths, w_keys, w_values):
    pool_pages, pool_scales = (
        lax.all_gather(latent_pages, "head", axis=1, tiled=True),
        lax.all_gather(page_scales, "head", axis=1, tiled=True),
    )
    full_keys, full_values = (
        lax.all_gather(w_keys, "ctx", axis=0, tiled=True),
        lax.all_gather(w_values, "ctx", axis=0, tiled=True),
    )
    latent_width = full_keys.shape[0]
    up_keys = full_keys.reshape(latent_width, -1)
    up_values = full_values.reshape(latent_width, -1)
    span_query = queries[0]
    own_pages = pool_pages[0]
    own_scales = pool_scales[0]
    own_table = page_table[0]
    row_count = span_query.shape[0]
    block_keys = 2 * own_pages.shape[1]
    own_length = lengths[0]
    block_count = (own_length + block_keys - 1) // block_keys

    def own_fetch(block_index):
        pool_slots = lax.dynamic_slice_in_dim(own_table, 2 * block_index, 2)
        return (
            jnp.take(own_pages, pool_slots, axis=0),
            jnp.take(own_scales, pool_slots, axis=0),
            block_index * block_keys,
        )

    row_top, row_total, summed = sweep(
        span_query, own_length - row_count, 0, block_count, own_fetch, up_keys, up_values
    )
    return finish(row_total, summed)


def gather_attend(
    shard_columns, q_in, pages_in, scales_in, table_in, wk_in, wv_in, length_in, out,
    q_rx, q_own, k_all, pages, scales, table, t_own, t_rx, wk_raw, wv_raw, w_all, rot, late,
    stage, own_sem, core_send, core_recv, relay_send, relay_recv, k_send, k_recv, t_send, t_recv,
    q_send, q_recv, z_send, z_recv, x_send, x_recv, f_send, f_recv,
    r_send, g_send, o_send, o_recv
):
    chunk_count = w_all.shape[0]
    latent_rows = w_all.shape[3]
    latent_width = w_all.shape[2] * latent_rows
    span = q_in.shape[-1]
    nope = w_all.shape[-1] // 2
    rope = q_in.shape[-2] - nope
    half_heads = chunk_count * PAIR
    page_count, page = k_all.shape[2], k_all.shape[3]
    key_count = 2 * page_count * page
    group_count = scales.shape[1]
    group_width = latent_width // group_count
    scale = math.log2(math.e) / math.sqrt(nope + rope)
    y, ctx, core = lax.axis_index("groups"), lax.axis_index("ctx"), lax.axis_index("head")
    row, side = ctx // 2, lax.rem(ctx, 2)
    last = shard_columns - 1
    y_peer = {"groups": 1 - y}
    core_peer = {"head": 1 - core}
    x_peer = {"ctx": 2 * row + 1 - side}
    partner = row + 1 - 2 * lax.rem(row, 2)

    def column(other):
        return {"ctx": 2 * other + side}

    def exists(other):
        return jnp.logical_and(other >= 0, other <= last)

    def local(source, target, index):
        return pltpu.make_async_copy(source, target, own_sem.at[index])

    heads_here = pl.ds(pl.multiple_of(y * half_heads, half_heads), half_heads)
    loads = [
        local(wk_in.at[:, heads_here], wk_raw, 0),
        local(wv_in.at[:, heads_here], wv_raw, 1),
        local(pages_in, pages, 2),
        local(scales_in, scales, 3),
        local(table_in, table, 4),
        local(q_in.at[y], q_own, 5),
    ]
    for load in loads:
        load.start()

    barrier = pltpu.get_barrier_semaphore()
    peers = [y_peer, core_peer, x_peer]
    peers += [column(lax.rem(row + d, shard_columns)) for d in range(1, shard_columns)]
    for peer in peers:
        pl.semaphore_signal(barrier, inc=1, device_id=peer, device_id_type=MESH)

    def remote(source, target, send, recv, peer):
        return pltpu.make_async_remote_copy(
            src_ref=source, dst_ref=target, send_sem=send, recv_sem=recv,
            device_id=peer, device_id_type=MESH,
        )

    def moved(c, source_row, source_side, send, recv, peer):
        block = w_all.at[c, :, 2 * source_row + source_side]
        return remote(block, block, send, recv, peer)

    k_mine = k_all.at[y, core]
    k_copy = remote(k_mine, k_mine, k_send, k_recv, y_peer)
    t_copy = remote(t_own, t_rx, t_send, t_recv, y_peer)
    core_copy = remote(k_mine, k_mine, core_send, core_recv, core_peer)
    k_other = k_all.at[1 - y, core]
    relay_copy = remote(k_other, k_other, relay_send, relay_recv, core_peer)

    def q_copy(c):
        return remote(q_in.at[1 - y, c], q_rx.at[c], q_send, q_recv.at[c], y_peer)

    hops = [(distance, step) for distance in (1, 2) for step in (1, -1)]

    def z_copy(c, index):
        distance, step = hops[index]
        return moved(
            c, row, side, z_send.at[index], z_recv.at[c, row], column(row + step * distance)
        )

    def z_arrival(c, source):
        return moved(c, source, side, z_send.at[0], z_recv.at[c, source], x_peer)

    def r_copy(c, step):
        source = row + 2 * step
        return moved(c, source, side, r_send, z_recv.at[c, source], column(row - step))

    def x_copy(c):
        return moved(c, row, side, x_send, x_recv.at[c], x_peer)

    def x_arrival(c):
        return moved(c, row, 1 - side, x_send, x_recv.at[c], x_peer)

    def f_copy(c, source):
        return moved(c, source, side, f_send.at[source], f_recv.at[c], x_peer)

    def f_arrivals(c):
        blocks = w_all.at[c, :, 0:last]
        return remote(blocks, blocks, x_send, f_recv.at[c], x_peer)

    def sent(count, semaphore):
        blocks = w_all.at[0:count, :, 0]
        return remote(blocks, blocks, semaphore, x_recv.at[0], x_peer)

    def g_copy(c):
        return moved(c, row, 1 - side, g_send, f_recv.at[c], column(partner))

    def by_z(c):
        return c >= chunk_count // 2

    def over_x(c, source):
        return jnp.logical_or(jnp.logical_not(by_z(c)), source != partner)

    def o_copy(c, h):
        return remote(stage.at[c, h], out.at[y, c, h], o_send, o_recv, y_peer)

    def send_own(c):
        for index, (distance, step) in enumerate(hops):
            @pl.when(exists(row + step * distance))
            def _():
                z_copy(c, index).start()

        x_copy(c).start()

    loads[0].wait()
    loads[1].wait()
    keys_by_head = jnp.swapaxes(wk_raw[...], 0, 1)
    values_by_head = jnp.swapaxes(wv_raw[...], 0, 1)
    for c in range(chunk_count):
        for h in range(PAIR):
            w_all[c, h, ctx, :, :nope] = keys_by_head[c * PAIR + h]
            w_all[c, h, ctx, :, nope:] = values_by_head[c * PAIR + h]

    pl.semaphore_wait(barrier, len(peers))
    for c in range(AHEAD):
        send_own(c)

    loads[2].wait()
    loads[3].wait()
    columns = jnp.transpose(
        scales[...].astype(jnp.float32).reshape(page_count * group_count, page)
    )
    for p in range(page_count):
        for g in range(group_count):
            part = pl.ds(g * group_width, group_width)
            at = p * group_count + g
            codes = pages[p, :, part].astype(jnp.float32)
            k_all[y, core, p, :, part] = (codes * columns[:, at : at + 1]).astype(jnp.bfloat16)
        k_all[y, core, p, :, latent_width:] = pages[p, :, latent_width:]
    k_copy.start()
    core_copy.start()
    loads[4].wait()
    slots = 2 * page_count
    slot = lax.broadcasted_iota(jnp.int32, (slots, slots), 0)
    place = lax.broadcasted_iota(jnp.int32, (slots, slots), 1)
    order = jnp.sum(jnp.where(table[...] == slot, place, 0), axis=1, keepdims=True)
    t_own[...] = jnp.broadcast_to(order * page - (length_in[0] - span), t_own.shape)
    t_copy.start()

    def send_queries(c, carry):
        q_copy(c).start()
        return carry

    lax.fori_loop(0, chunk_count, send_queries, 0)
    loads[5].wait()

    def settle():
        t_copy.wait_recv()
        core_copy.wait_recv()
        relay_copy.wait_recv()
        offset = lax.broadcasted_iota(jnp.int32, (page, span), 0)
        offset = offset - lax.broadcasted_iota(jnp.int32, (page, span), 1)
        for request, t_ref in ((y, t_own), (1 - y, t_rx)):
            rot[request] = k_all[request, :, :, :, latent_width:].reshape(key_count, rope)
            behind = jnp.concatenate([t_ref[p : p + 1] + offset for p in range(slots)], axis=0)
            late[request] = jnp.where(behind <= 0, 0.0, NEGATIVE)

    def attend(c, h, request, q_ref):
        latent = k_all[request, :, :, :, :latent_width].reshape(key_count, latent_width)
        weight = w_all[c, h].reshape(latent_width, -1)
        up = jnp.dot(latent, weight, preferred_element_type=jnp.float32).astype(jnp.bfloat16)
        keys = jnp.concatenate([up[:, :nope], rot[request]], axis=1)
        scores = jnp.dot(keys, q_ref[c, h], preferred_element_type=jnp.float32)
        scores = scores * scale + late[request]
        top = jnp.max(scores, axis=0, keepdims=True)
        raw = jnp.exp2(scores - top)
        total = jnp.sum(raw, axis=0, keepdims=True)
        summed = lax.dot_general(
            up[:, nope:], raw.astype(jnp.bfloat16), (((0,), (0,)), ((), ())),
            preferred_element_type=jnp.float32,
        )
        return jnp.transpose(summed * (1.0 / total)).astype(jnp.bfloat16)

    def pass_on(c, distance):
        for step in (1, -1):
            source = row + step * distance

            @pl.when(exists(source))
            def _():
                z_arrival(c, source).wait_recv()
                if distance == 2:
                    @pl.when(exists(row - step))
                    def _():
                        r_copy(c, step).start()

                @pl.when(over_x(c, source))
                def _():
                    f_copy(c, source).start()

    def advance(c, carry):
        @pl.when(c + AHEAD < chunk_count)
        def _():
            send_own(c + AHEAD)

        sending = c < chunk_count
        ready = c >= LAG
        b = jnp.maximum(c - LAG, 0)
        for unit in range(2 * PAIR):
            if unit == 0:
                @pl.when(sending)
                def _():
                    pass_on(c, 1)

            if unit == 1:
                @pl.when(sending)
                def _():
                    pass_on(c, 2)

            if unit == 2:
                @pl.when(sending)
                def _():
                    x_arrival(c).wait_recv()

                    @pl.when(by_z(c))
                    def _():
                        g_copy(c).start()


            if unit == 0:
                @pl.when(c == LAG)
                def _():
                    settle()

            @pl.when(ready)
            def _():
                if unit == 0:
                    f_arrivals(b).wait_recv()
                    q_copy(b).wait_recv()
                h = unit % PAIR
                if unit < PAIR:
                    stage[b, h] = attend(b, h, 1 - y, q_rx)
                    o_copy(b, h).start()
                else:
                    out[y, b, h] = attend(b, h, y, q_own)

        @pl.when(sending)
        def _():
            pass_on(c, 3)

        @pl.when(c == LAG - 1)
        def _():
            k_copy.wait_recv()
            relay_copy.start()

        return carry

    lax.fori_loop(0, chunk_count + LAG, advance, 0)
    k_copy.wait_send()
    t_copy.wait_send()
    core_copy.wait_send()
    relay_copy.wait_send()

    direct = chunk_count // 2
    q_all = q_in.at[1 - y]
    remote(q_all, q_all, q_send, q_recv.at[0], y_peer).wait_send()
    sent(chunk_count, x_send).wait_send()
    sent(direct, g_send).wait_send()
    for index, (distance, step) in enumerate(hops):
        @pl.when(exists(row + step * distance))
        def _():
            sent(chunk_count, z_send.at[index]).wait_send()

        if distance == 2:
            @pl.when(jnp.logical_and(exists(row + 2 * step), exists(row - step)))
            def _():
                sent(chunk_count, r_send).wait_send()

    for d in range(1, shard_columns):
        other = lax.rem(row + d, shard_columns)

        @pl.when(other == partner)
        def _():
            sent(chunk_count - direct, f_send.at[other]).wait_send()

        @pl.when(other != partner)
        def _():
            sent(chunk_count, f_send.at[other]).wait_send()

    remote(stage, out.at[y], o_send, o_recv, y_peer).wait()


def shared_on_device(
    shards, queries, latent_pages, page_scales, page_table, lengths, w_keys, w_values
):
    _, span, heads, _ = queries.shape
    latent_rows, _, nope = w_keys.shape
    _, slots, page, width = latent_pages.shape
    latent_width = latent_rows * shards
    rope = width - latent_width
    groups = page_scales.shape[2]
    chunks = heads // (2 * PAIR)
    pool = page_table.shape[1]
    columns = shards // 2
    half = heads // 2
    q_in = jnp.transpose(queries[0], (1, 2, 0)).reshape(2, chunks, PAIR, -1, span)
    operands = (
        q_in, latent_pages[0], page_scales[0], page_table, w_keys, w_values
    )
    dma, vmem = pltpu.SemaphoreType.DMA, pltpu.VMEM
    bf16, int32 = jnp.bfloat16, jnp.int32
    out = pl.pallas_call(
        functools.partial(gather_attend, columns),
        out_shape=vmem((2, chunks, PAIR, span, nope), bf16),
        in_specs=[pl.BlockSpec(memory_space=pltpu.HBM)] * 6
        + [pl.BlockSpec(memory_space=pltpu.SMEM)],
        out_specs=pl.BlockSpec(memory_space=vmem),
        scratch_shapes=[
            vmem(q_in.shape[1:], bf16),
            vmem(q_in.shape[1:], bf16),
            vmem((2, 2, slots, page, width), bf16),
            vmem((slots, page, width), bf16),
            vmem((slots, groups, page), bf16),
            vmem((1, pool), int32),
            vmem((pool, span), int32),
            vmem((pool, span), int32),
            vmem((latent_rows, half, nope), bf16),
            vmem((latent_rows, half, nope), bf16),
            vmem((chunks, PAIR, shards, latent_rows, 2 * nope), bf16),
            vmem((2, pool * page, rope), bf16),
            vmem((2, pool * page, span), jnp.float32),
            vmem((chunks, PAIR, span, nope), bf16),
            dma((6,)), dma, dma, dma, dma, dma, dma, dma, dma,
            dma, dma((chunks,)),
            dma((4,)), dma((chunks, columns)),
            dma, dma((chunks,)),
            dma((columns,)), dma((chunks,)),
            dma, dma, dma, dma,
        ],
        compiler_params=pltpu.CompilerParams(
            collective_id=0, has_side_effects=True, vmem_limit_bytes=48 * 1024 * 1024
        ),
    )(*(pltpu.with_memory_space_constraint(x, pltpu.HBM) for x in operands), lengths)
    return jnp.swapaxes(out.reshape(heads, span, nope), 0, 1)[None]


def body_for(mesh, queries, latent_pages, page_scales, page_table, lengths, w_keys, w_values):
    args = (queries, latent_pages, page_scales, page_table, lengths, w_keys, w_values)
    shards = mesh.shape["ctx"]
    rope = latent_pages.shape[3] - w_keys.shape[0] * shards
    fits = (
        mesh.shape["groups"] == 2 and mesh.shape["head"] == 2 and shards == 8
        and w_keys.shape[0] % 16 == 0 and queries.shape[2] % 16 == 0
        and w_keys.shape == w_values.shape and 2 * rope == w_keys.shape[2]
    )
    if fits:
        return shared_on_device(shards, *args)
    return on_device(*args)


def solution(mesh):
    return jax.shard_map(
        functools.partial(body_for, mesh),
        mesh=mesh,
        in_specs=(
            P(("groups", "ctx"), None, "head", None),
            P(("groups", "ctx"), "head", None, None),
            P(("groups", "ctx"), "head", None, None),
            P(("groups", "ctx"), None),
            P(("groups", "ctx")),
            P("ctx", "head", None),
            P("ctx", "head", None),
        ),
        out_specs=P(("groups", "ctx"), None, "head", None),
        check_vma=False,
    )
```

```python
import functools
import math

import jax
import jax.numpy as jnp
from jax import lax
from jax.experimental import pallas as pl
from jax.experimental.pallas import tpu as pltpu
from jax.sharding import PartitionSpec as P

NEGATIVE = -1e30
MESH = pl.DeviceIdType.MESH
PAIR = 2
LAG = 2
AHEAD = 3
INNER = 0
OUTER = 4


def attend_block(
    running, span_query, page_data, page_factor, first_key, row_offset, up_keys, up_values
):
    row_top, row_total, summed = running
    latent_width = up_keys.shape[0]
    group_count = page_factor.shape[1]
    page_rows = page_data.shape[1]
    key_count = page_data.shape[0] * page_rows
    head_count = span_query.shape[1]
    code_values = page_data[:, :, :latent_width].astype(jnp.float32)
    code_values = code_values.reshape(
        page_data.shape[0], page_rows, group_count, latent_width // group_count
    )
    factor = jnp.swapaxes(page_factor, 1, 2).astype(jnp.float32)[..., None]
    latent = (code_values * factor).reshape(key_count, latent_width).astype(jnp.bfloat16)
    rotary = page_data[:, :, latent_width:].reshape(key_count, -1)
    key_nope = jnp.dot(latent, up_keys, preferred_element_type=jnp.float32).astype(jnp.bfloat16)
    key_nope = key_nope.reshape(key_count, head_count, -1)
    value_rows = jnp.dot(latent, up_values, preferred_element_type=jnp.float32).astype(jnp.bfloat16)
    value_rows = value_rows.reshape(key_count, head_count, -1)
    nope_width = key_nope.shape[2]
    scores = jnp.einsum(
        "chn,khn->hck", span_query[:, :, :nope_width], key_nope, preferred_element_type=jnp.float32
    )
    scores = scores + jnp.einsum(
        "chr,kr->hck", span_query[:, :, nope_width:], rotary, preferred_element_type=jnp.float32
    )
    scores = scores * (1.0 / math.sqrt(span_query.shape[2]))
    row_position = lax.broadcasted_iota(jnp.int32, (span_query.shape[0], key_count), 0)
    key_position = first_key + lax.broadcasted_iota(jnp.int32, (span_query.shape[0], key_count), 1)
    visible = (key_position <= row_offset + row_position)[None]
    new_top = jnp.maximum(row_top, jnp.max(jnp.where(visible, scores, NEGATIVE), axis=2))
    raw_weight = jnp.where(visible, jnp.exp(scores - new_top[..., None]), 0.0)
    rescale = jnp.exp(row_top - new_top)
    row_total = row_total * rescale + jnp.sum(raw_weight, axis=2)
    weights = raw_weight.astype(jnp.bfloat16)
    summed = summed * jnp.swapaxes(rescale, 0, 1)[..., None] + jnp.einsum(
        "hck,khv->chv", weights, value_rows, preferred_element_type=jnp.float32
    )
    return (new_top, row_total, summed)


def sweep(span_query, row_offset, first_block, stop_block, fetch, up_keys, up_values):
    row_count = span_query.shape[0]
    head_count = span_query.shape[1]
    value_width = up_values.shape[1] // head_count
    initial = (
        jnp.full((head_count, row_count), NEGATIVE, jnp.float32),
        jnp.zeros((head_count, row_count), jnp.float32),
        jnp.zeros((row_count, head_count, value_width), jnp.float32),
    )

    def advance(block_index, running):
        page_data, page_factor, first_key = fetch(block_index)
        return attend_block(
            running, span_query, page_data, page_factor, first_key, row_offset, up_keys, up_values
        )

    return lax.fori_loop(first_block, stop_block, advance, initial)


def finish(row_total, summed):
    return (summed / jnp.swapaxes(row_total, 0, 1)[..., None]).astype(jnp.bfloat16)[None]


def on_device(queries, latent_pages, page_scales, page_table, lengths, w_keys, w_values):
    pool_pages, pool_scales = (
        lax.all_gather(latent_pages, "head", axis=1, tiled=True),
        lax.all_gather(page_scales, "head", axis=1, tiled=True),
    )
    full_keys, full_values = (
        lax.all_gather(w_keys, "ctx", axis=0, tiled=True),
        lax.all_gather(w_values, "ctx", axis=0, tiled=True),
    )
    latent_width = full_keys.shape[0]
    up_keys = full_keys.reshape(latent_width, -1)
    up_values = full_values.reshape(latent_width, -1)
    span_query = queries[0]
    own_pages = pool_pages[0]
    own_scales = pool_scales[0]
    own_table = page_table[0]
    row_count = span_query.shape[0]
    block_keys = 2 * own_pages.shape[1]
    own_length = lengths[0]
    block_count = (own_length + block_keys - 1) // block_keys

    def own_fetch(block_index):
        pool_slots = lax.dynamic_slice_in_dim(own_table, 2 * block_index, 2)
        return (
            jnp.take(own_pages, pool_slots, axis=0),
            jnp.take(own_scales, pool_slots, axis=0),
            block_index * block_keys,
        )

    row_top, row_total, summed = sweep(
        span_query, own_length - row_count, 0, block_count, own_fetch, up_keys, up_values
    )
    return finish(row_total, summed)


def gather_attend(
    shard_columns, q_in, pages_in, scales_in, table_in, wk_in, wv_in, length_in, out,
    q_rx, q_own, k_all, pages, scales, table, t_own, t_rx, wk_raw, wv_raw, w_all, rot, late,
    stage, own_sem, core_send, core_recv, relay_send, relay_recv, k_send, k_recv, t_send, t_recv,
    q_send, q_recv, z_send, z_recv, x_send, x_recv, f_send, f_recv,
    r_send, g_send, o_send, o_recv
):
    chunk_count = w_all.shape[0]
    latent_rows = w_all.shape[3]
    latent_width = w_all.shape[2] * latent_rows
    span = q_in.shape[-1]
    nope = w_all.shape[-1] // 2
    rope = q_in.shape[-2] - nope
    half_heads = chunk_count * PAIR
    page_count, page = k_all.shape[2], k_all.shape[3]
    key_count = 2 * page_count * page
    group_count = scales.shape[1]
    group_width = latent_width // group_count
    scale = math.log2(math.e) / math.sqrt(nope + rope)
    y, ctx, core = lax.axis_index("groups"), lax.axis_index("ctx"), lax.axis_index("head")
    row, side = ctx // 2, lax.rem(ctx, 2)
    last = shard_columns - 1
    y_peer = {"groups": 1 - y}
    core_peer = {"head": 1 - core}
    x_peer = {"ctx": 2 * row + 1 - side}
    partner = row + 1 - 2 * lax.rem(row, 2)

    def column(other):
        return {"ctx": 2 * other + side}

    def exists(other):
        return jnp.logical_and(other >= 0, other <= last)

    def local(source, target, index):
        return pltpu.make_async_copy(source, target, own_sem.at[index])

    heads_here = pl.ds(pl.multiple_of(y * half_heads, half_heads), half_heads)
    loads = [
        local(wk_in.at[:, heads_here], wk_raw, 0),
        local(wv_in.at[:, heads_here], wv_raw, 1),
        local(pages_in, pages, 2),
        local(scales_in, scales, 3),
        local(table_in, table, 4),
        local(q_in.at[y], q_own, 5),
    ]
    for load in loads:
        load.start()

    barrier = pltpu.get_barrier_semaphore()
    peers = [y_peer, core_peer, x_peer]
    peers += [column(lax.rem(row + d, shard_columns)) for d in range(1, shard_columns)]
    for peer in peers:
        pl.semaphore_signal(barrier, inc=1, device_id=peer, device_id_type=MESH)

    def remote(source, target, send, recv, peer):
        return pltpu.make_async_remote_copy(
            src_ref=source, dst_ref=target, send_sem=send, recv_sem=recv,
            device_id=peer, device_id_type=MESH,
        )

    def moved(c, source_row, source_side, send, recv, peer):
        block = w_all.at[c, :, 2 * source_row + source_side]
        return remote(block, block, send, recv, peer)

    k_mine = k_all.at[y, core]
    k_copy = remote(k_mine, k_mine, k_send, k_recv, y_peer)
    t_copy = remote(t_own, t_rx, t_send, t_recv, y_peer)
    core_copy = remote(k_mine, k_mine, core_send, core_recv, core_peer)
    k_other = k_all.at[1 - y, core]
    relay_copy = remote(k_other, k_other, relay_send, relay_recv, core_peer)

    def q_copy(c):
        return remote(q_in.at[1 - y, c], q_rx.at[c], q_send, q_recv.at[c], y_peer)

    hops = [(distance, step) for distance in (1, 2) for step in (1, -1)]

    def z_copy(c, index):
        distance, step = hops[index]
        return moved(
            c, row, side, z_send.at[index], z_recv.at[c, row], column(row + step * distance)
        )

    def z_arrival(c, source):
        return moved(c, source, side, z_send.at[0], z_recv.at[c, source], x_peer)

    def r_copy(c, step):
        source = row + 2 * step
        return moved(c, source, side, r_send, z_recv.at[c, source], column(row - step))

    def two(c, shard, send, recv, peer):
        blocks = w_all.at[pl.ds(c, 2), :, shard]
        return remote(blocks, blocks, send, recv, peer)

    def x_copy(c):
        return two(c, ctx, x_send, x_recv.at[c // 2], x_peer)

    def x_arrival(c):
        return two(c, 2 * row + 1 - side, x_send, x_recv.at[c // 2], x_peer)

    def f_copy(c, source):
        return moved(c, source, side, f_send.at[source], f_recv.at[c], x_peer)

    def f_arrivals(c):
        blocks = w_all.at[c, :, 0:last]
        return remote(blocks, blocks, x_send, f_recv.at[c], x_peer)

    def sent(count, semaphore):
        blocks = w_all.at[0:count, :, 0]
        return remote(blocks, blocks, semaphore, x_recv.at[0], x_peer)

    def g_copy(c):
        return moved(c, row, 1 - side, g_send, f_recv.at[c], column(partner))

    def inner(r):
        return jnp.logical_and(r > 0, r < last)

    def first_by_z(r):
        return jnp.where(inner(r), INNER, OUTER)

    def by_z(c, r):
        return c >= first_by_z(r)

    def over_x(c, source):
        return jnp.logical_or(jnp.logical_not(by_z(c, row)), source != partner)

    def o_copy(c, h):
        return remote(stage.at[c, h], out.at[y, c, h], o_send, o_recv, y_peer)

    def send_own(c):
        for index, (distance, step) in enumerate(hops):
            @pl.when(exists(row + step * distance))
            def _():
                z_copy(c, index).start()

        @pl.when(lax.rem(c, 2) == 0)
        def _():
            x_copy(c).start()

    loads[0].wait()
    loads[1].wait()
    keys_by_head = jnp.swapaxes(wk_raw[...], 0, 1)
    values_by_head = jnp.swapaxes(wv_raw[...], 0, 1)
    for c in range(chunk_count):
        for h in range(PAIR):
            w_all[c, h, ctx, :, :nope] = keys_by_head[c * PAIR + h]
            w_all[c, h, ctx, :, nope:] = values_by_head[c * PAIR + h]

    pl.semaphore_wait(barrier, len(peers))
    for c in range(AHEAD):
        send_own(c)

    loads[2].wait()
    loads[3].wait()
    columns = jnp.transpose(
        scales[...].astype(jnp.float32).reshape(page_count * group_count, page)
    )
    for p in range(page_count):
        for g in range(group_count):
            part = pl.ds(g * group_width, group_width)
            at = p * group_count + g
            codes = pages[p, :, part].astype(jnp.float32)
            k_all[y, core, p, :, part] = (codes * columns[:, at : at + 1]).astype(jnp.bfloat16)
        k_all[y, core, p, :, latent_width:] = pages[p, :, latent_width:]
    k_copy.start()
    core_copy.start()
    loads[4].wait()
    slots = 2 * page_count
    slot = lax.broadcasted_iota(jnp.int32, (slots, slots), 0)
    place = lax.broadcasted_iota(jnp.int32, (slots, slots), 1)
    order = jnp.sum(jnp.where(table[...] == slot, place, 0), axis=1, keepdims=True)
    t_own[...] = jnp.broadcast_to(order * page - (length_in[0] - span), t_own.shape)
    t_copy.start()

    def send_queries(c, carry):
        q_copy(c).start()
        return carry

    lax.fori_loop(0, chunk_count, send_queries, 0)
    loads[5].wait()

    def settle():
        t_copy.wait_recv()
        core_copy.wait_recv()
        relay_copy.wait_recv()
        offset = lax.broadcasted_iota(jnp.int32, (page, span), 0)
        offset = offset - lax.broadcasted_iota(jnp.int32, (page, span), 1)
        for request, t_ref in ((y, t_own), (1 - y, t_rx)):
            rot[request] = k_all[request, :, :, :, latent_width:].reshape(key_count, rope)
            behind = jnp.concatenate([t_ref[p : p + 1] + offset for p in range(slots)], axis=0)
            late[request] = jnp.where(behind <= 0, 0.0, NEGATIVE)

    def attend(c, h, request, q_ref):
        latent = k_all[request, :, :, :, :latent_width].reshape(key_count, latent_width)
        weight = w_all[c, h].reshape(latent_width, -1)
        up = jnp.dot(latent, weight, preferred_element_type=jnp.float32).astype(jnp.bfloat16)
        keys = jnp.concatenate([up[:, :nope], rot[request]], axis=1)
        scores = jnp.dot(keys, q_ref[c, h], preferred_element_type=jnp.float32)
        scores = scores * scale + late[request]
        top = jnp.max(scores, axis=0, keepdims=True)
        raw = jnp.exp2(scores - top)
        total = jnp.sum(raw, axis=0, keepdims=True)
        summed = lax.dot_general(
            up[:, nope:], raw.astype(jnp.bfloat16), (((0,), (0,)), ((), ())),
            preferred_element_type=jnp.float32,
        )
        return jnp.transpose(summed * (1.0 / total)).astype(jnp.bfloat16)

    def pass_on(c, distance):
        for step in (1, -1):
            source = row + step * distance

            @pl.when(exists(source))
            def _():
                z_arrival(c, source).wait_recv()
                if distance == 2:
                    @pl.when(exists(row - step))
                    def _():
                        r_copy(c, step).start()

                @pl.when(over_x(c, source))
                def _():
                    f_copy(c, source).start()

    def advance(c, carry):
        @pl.when(c + AHEAD < chunk_count)
        def _():
            send_own(c + AHEAD)

        sending = c < chunk_count
        ready = c >= LAG
        b = jnp.maximum(c - LAG, 0)
        for unit in range(2 * PAIR):
            if unit == 0:
                @pl.when(sending)
                def _():
                    pass_on(c, 1)

            if unit == 1:
                @pl.when(sending)
                def _():
                    pass_on(c, 2)
                    @pl.when(lax.rem(c, 2) == 0)
                    def _():
                        x_arrival(c).wait_recv()

                    @pl.when(by_z(c, partner))
                    def _():
                        g_copy(c).start()


            if unit == 0:
                @pl.when(c == LAG)
                def _():
                    settle()

            @pl.when(ready)
            def _():
                if unit == 0:
                    f_arrivals(b).wait_recv()
                    q_copy(b).wait_recv()
                h = unit % PAIR
                if unit < PAIR:
                    stage[b, h] = attend(b, h, 1 - y, q_rx)
                    o_copy(b, h).start()
                else:
                    out[y, b, h] = attend(b, h, y, q_own)

        @pl.when(sending)
        def _():
            pass_on(c, 3)

        @pl.when(c == LAG - 1)
        def _():
            k_copy.wait_recv()
            relay_copy.start()

        return carry

    lax.fori_loop(0, chunk_count + LAG, advance, 0)
    k_copy.wait_send()
    t_copy.wait_send()
    core_copy.wait_send()
    relay_copy.wait_send()

    q_all = q_in.at[1 - y]
    remote(q_all, q_all, q_send, q_recv.at[0], y_peer).wait_send()
    sent(chunk_count, x_send).wait_send()
    for inside, first in ((True, INNER), (False, OUTER)):
        @pl.when(inner(partner) == inside)
        def _():
            sent(chunk_count - first, g_send).wait_send()

    for index, (distance, step) in enumerate(hops):
        @pl.when(exists(row + step * distance))
        def _():
            sent(chunk_count, z_send.at[index]).wait_send()

        if distance == 2:
            @pl.when(jnp.logical_and(exists(row + 2 * step), exists(row - step)))
            def _():
                sent(chunk_count, r_send).wait_send()

    for d in range(1, shard_columns):
        other = lax.rem(row + d, shard_columns)

        for inside, first in ((True, INNER), (False, OUTER)):
            if first > 0:
                @pl.when(jnp.logical_and(other == partner, inner(row) == inside))
                def _():
                    sent(first, f_send.at[other]).wait_send()

        @pl.when(other != partner)
        def _():
            sent(chunk_count, f_send.at[other]).wait_send()

    remote(stage, out.at[y], o_send, o_recv, y_peer).wait()


def shared_on_device(
    shards, queries, latent_pages, page_scales, page_table, lengths, w_keys, w_values
):
    _, span, heads, _ = queries.shape
    latent_rows, _, nope = w_keys.shape
    _, slots, page, width = latent_pages.shape
    latent_width = latent_rows * shards
    rope = width - latent_width
    groups = page_scales.shape[2]
    chunks = heads // (2 * PAIR)
    pool = page_table.shape[1]
    columns = shards // 2
    half = heads // 2
    q_in = jnp.transpose(queries[0], (1, 2, 0)).reshape(2, chunks, PAIR, -1, span)
    operands = (
        q_in, latent_pages[0], page_scales[0], page_table, w_keys, w_values
    )
    dma, vmem = pltpu.SemaphoreType.DMA, pltpu.VMEM
    bf16, int32 = jnp.bfloat16, jnp.int32
    out = pl.pallas_call(
        functools.partial(gather_attend, columns),
        out_shape=vmem((2, chunks, PAIR, span, nope), bf16),
        in_specs=[pl.BlockSpec(memory_space=pltpu.HBM)] * 6
        + [pl.BlockSpec(memory_space=pltpu.SMEM)],
        out_specs=pl.BlockSpec(memory_space=vmem),
        scratch_shapes=[
            vmem(q_in.shape[1:], bf16),
            vmem(q_in.shape[1:], bf16),
            vmem((2, 2, slots, page, width), bf16),
            vmem((slots, page, width), bf16),
            vmem((slots, groups, page), bf16),
            vmem((1, pool), int32),
            vmem((pool, span), int32),
            vmem((pool, span), int32),
            vmem((latent_rows, half, nope), bf16),
            vmem((latent_rows, half, nope), bf16),
            vmem((chunks, PAIR, shards, latent_rows, 2 * nope), bf16),
            vmem((2, pool * page, rope), bf16),
            vmem((2, pool * page, span), jnp.float32),
            vmem((chunks, PAIR, span, nope), bf16),
            dma((6,)), dma, dma, dma, dma, dma, dma, dma, dma,
            dma, dma((chunks,)),
            dma((4,)), dma((chunks, columns)),
            dma, dma((chunks,)),
            dma((columns,)), dma((chunks,)),
            dma, dma, dma, dma,
        ],
        compiler_params=pltpu.CompilerParams(
            collective_id=0, has_side_effects=True, vmem_limit_bytes=48 * 1024 * 1024
        ),
    )(*(pltpu.with_memory_space_constraint(x, pltpu.HBM) for x in operands), lengths)
    return jnp.swapaxes(out.reshape(heads, span, nope), 0, 1)[None]


def body_for(mesh, queries, latent_pages, page_scales, page_table, lengths, w_keys, w_values):
    args = (queries, latent_pages, page_scales, page_table, lengths, w_keys, w_values)
    shards = mesh.shape["ctx"]
    rope = latent_pages.shape[3] - w_keys.shape[0] * shards
    fits = (
        mesh.shape["groups"] == 2 and mesh.shape["head"] == 2 and shards == 8
        and w_keys.shape[0] % 16 == 0 and queries.shape[2] % 16 == 0
        and w_keys.shape == w_values.shape and 2 * rope == w_keys.shape[2]
    )
    if fits:
        return shared_on_device(shards, *args)
    return on_device(*args)


def solution(mesh):
    return jax.shard_map(
        functools.partial(body_for, mesh),
        mesh=mesh,
        in_specs=(
            P(("groups", "ctx"), None, "head", None),
            P(("groups", "ctx"), "head", None, None),
            P(("groups", "ctx"), "head", None, None),
            P(("groups", "ctx"), None),
            P(("groups", "ctx")),
            P("ctx", "head", None),
            P("ctx", "head", None),
        ),
        out_specs=P(("groups", "ctx"), None, "head", None),
        check_vma=False,
    )
```

```python
import functools
import math

import jax
import jax.numpy as jnp
from jax import lax
from jax.experimental import pallas as pl
from jax.experimental.pallas import tpu as pltpu
from jax.sharding import PartitionSpec as P

NEGATIVE = -1e30
MESH = pl.DeviceIdType.MESH
PAIR = 2
LAG = 2
AHEAD = 4
INNER = 0
OUTER = 4


def attend_block(
    running, span_query, page_data, page_factor, first_key, row_offset, up_keys, up_values
):
    row_top, row_total, summed = running
    latent_width = up_keys.shape[0]
    group_count = page_factor.shape[1]
    page_rows = page_data.shape[1]
    key_count = page_data.shape[0] * page_rows
    head_count = span_query.shape[1]
    code_values = page_data[:, :, :latent_width].astype(jnp.float32)
    code_values = code_values.reshape(
        page_data.shape[0], page_rows, group_count, latent_width // group_count
    )
    factor = jnp.swapaxes(page_factor, 1, 2).astype(jnp.float32)[..., None]
    latent = (code_values * factor).reshape(key_count, latent_width).astype(jnp.bfloat16)
    rotary = page_data[:, :, latent_width:].reshape(key_count, -1)
    key_nope = jnp.dot(latent, up_keys, preferred_element_type=jnp.float32).astype(jnp.bfloat16)
    key_nope = key_nope.reshape(key_count, head_count, -1)
    value_rows = jnp.dot(latent, up_values, preferred_element_type=jnp.float32).astype(jnp.bfloat16)
    value_rows = value_rows.reshape(key_count, head_count, -1)
    nope_width = key_nope.shape[2]
    scores = jnp.einsum(
        "chn,khn->hck", span_query[:, :, :nope_width], key_nope, preferred_element_type=jnp.float32
    )
    scores = scores + jnp.einsum(
        "chr,kr->hck", span_query[:, :, nope_width:], rotary, preferred_element_type=jnp.float32
    )
    scores = scores * (1.0 / math.sqrt(span_query.shape[2]))
    row_position = lax.broadcasted_iota(jnp.int32, (span_query.shape[0], key_count), 0)
    key_position = first_key + lax.broadcasted_iota(jnp.int32, (span_query.shape[0], key_count), 1)
    visible = (key_position <= row_offset + row_position)[None]
    new_top = jnp.maximum(row_top, jnp.max(jnp.where(visible, scores, NEGATIVE), axis=2))
    raw_weight = jnp.where(visible, jnp.exp(scores - new_top[..., None]), 0.0)
    rescale = jnp.exp(row_top - new_top)
    row_total = row_total * rescale + jnp.sum(raw_weight, axis=2)
    weights = raw_weight.astype(jnp.bfloat16)
    summed = summed * jnp.swapaxes(rescale, 0, 1)[..., None] + jnp.einsum(
        "hck,khv->chv", weights, value_rows, preferred_element_type=jnp.float32
    )
    return (new_top, row_total, summed)


def sweep(span_query, row_offset, first_block, stop_block, fetch, up_keys, up_values):
    row_count = span_query.shape[0]
    head_count = span_query.shape[1]
    value_width = up_values.shape[1] // head_count
    initial = (
        jnp.full((head_count, row_count), NEGATIVE, jnp.float32),
        jnp.zeros((head_count, row_count), jnp.float32),
        jnp.zeros((row_count, head_count, value_width), jnp.float32),
    )

    def advance(block_index, running):
        page_data, page_factor, first_key = fetch(block_index)
        return attend_block(
            running, span_query, page_data, page_factor, first_key, row_offset, up_keys, up_values
        )

    return lax.fori_loop(first_block, stop_block, advance, initial)


def finish(row_total, summed):
    return (summed / jnp.swapaxes(row_total, 0, 1)[..., None]).astype(jnp.bfloat16)[None]


def on_device(queries, latent_pages, page_scales, page_table, lengths, w_keys, w_values):
    pool_pages, pool_scales = (
        lax.all_gather(latent_pages, "head", axis=1, tiled=True),
        lax.all_gather(page_scales, "head", axis=1, tiled=True),
    )
    full_keys, full_values = (
        lax.all_gather(w_keys, "ctx", axis=0, tiled=True),
        lax.all_gather(w_values, "ctx", axis=0, tiled=True),
    )
    latent_width = full_keys.shape[0]
    up_keys = full_keys.reshape(latent_width, -1)
    up_values = full_values.reshape(latent_width, -1)
    span_query = queries[0]
    own_pages = pool_pages[0]
    own_scales = pool_scales[0]
    own_table = page_table[0]
    row_count = span_query.shape[0]
    block_keys = 2 * own_pages.shape[1]
    own_length = lengths[0]
    block_count = (own_length + block_keys - 1) // block_keys

    def own_fetch(block_index):
        pool_slots = lax.dynamic_slice_in_dim(own_table, 2 * block_index, 2)
        return (
            jnp.take(own_pages, pool_slots, axis=0),
            jnp.take(own_scales, pool_slots, axis=0),
            block_index * block_keys,
        )

    row_top, row_total, summed = sweep(
        span_query, own_length - row_count, 0, block_count, own_fetch, up_keys, up_values
    )
    return finish(row_total, summed)


def gather_attend(
    shard_columns, q_in, pages_in, scales_in, table_in, wk_in, wv_in, length_in, out,
    q_rx, q_own, k_all, pages, scales, table, t_own, t_rx, wk_raw, wv_raw, w_all, rot, late,
    stage, own_sem, core_send, core_recv, relay_send, relay_recv, k_send, k_recv, t_send, t_recv,
    q_send, q_recv, z_send, z_recv, x_send, x_recv, f_send, f_recv,
    r_send, g_send, o_send, o_recv
):
    chunk_count = w_all.shape[0]
    latent_rows = w_all.shape[3]
    latent_width = w_all.shape[2] * latent_rows
    span = q_in.shape[-1]
    nope = w_all.shape[-1] // 2
    rope = q_in.shape[-2] - nope
    half_heads = chunk_count * PAIR
    page_count, page = k_all.shape[2], k_all.shape[3]
    key_count = 2 * page_count * page
    group_count = scales.shape[1]
    group_width = latent_width // group_count
    scale = math.log2(math.e) / math.sqrt(nope + rope)
    y, ctx, core = lax.axis_index("groups"), lax.axis_index("ctx"), lax.axis_index("head")
    row, side = ctx // 2, lax.rem(ctx, 2)
    last = shard_columns - 1
    y_peer = {"groups": 1 - y}
    core_peer = {"head": 1 - core}
    x_peer = {"ctx": 2 * row + 1 - side}
    partner = row + 1 - 2 * lax.rem(row, 2)

    def column(other):
        return {"ctx": 2 * other + side}

    def exists(other):
        return jnp.logical_and(other >= 0, other <= last)

    def local(source, target, index):
        return pltpu.make_async_copy(source, target, own_sem.at[index])

    heads_here = pl.ds(pl.multiple_of(y * half_heads, half_heads), half_heads)
    loads = [
        local(wk_in.at[:, heads_here], wk_raw, 0),
        local(wv_in.at[:, heads_here], wv_raw, 1),
        local(pages_in, pages, 2),
        local(scales_in, scales, 3),
        local(table_in, table, 4),
        local(q_in.at[y], q_own, 5),
    ]
    for load in loads:
        load.start()

    barrier = pltpu.get_barrier_semaphore()
    hops = [(distance, step) for distance in (1, 2) for step in (1, -1)]
    arrivals = 3
    for peer in (y_peer, core_peer, x_peer):
        pl.semaphore_signal(barrier, inc=1, device_id=peer, device_id_type=MESH)
    for distance, step in hops:
        here = exists(row + step * distance)
        arrivals = arrivals + here.astype(jnp.int32)

        @pl.when(here)
        def _():
            pl.semaphore_signal(
                barrier, inc=1, device_id=column(row + step * distance), device_id_type=MESH
            )

    def remote(source, target, send, recv, peer):
        return pltpu.make_async_remote_copy(
            src_ref=source, dst_ref=target, send_sem=send, recv_sem=recv,
            device_id=peer, device_id_type=MESH,
        )

    def moved(c, source_row, source_side, send, recv, peer):
        block = w_all.at[c, :, 2 * source_row + source_side]
        return remote(block, block, send, recv, peer)

    k_mine = k_all.at[y, core]
    k_copy = remote(k_mine, k_mine, k_send, k_recv, y_peer)
    t_copy = remote(t_own, t_rx, t_send, t_recv, y_peer)
    core_copy = remote(k_mine, k_mine, core_send, core_recv, core_peer)
    k_other = k_all.at[1 - y, core]
    relay_copy = remote(k_other, k_other, relay_send, relay_recv, core_peer)

    def q_copy(c):
        return remote(q_in.at[1 - y, c], q_rx.at[c], q_send, q_recv.at[c], y_peer)

    def z_copy(c, index):
        distance, step = hops[index]
        return moved(
            c, row, side, z_send.at[index], z_recv.at[c, row], column(row + step * distance)
        )

    def z_arrival(c, source):
        return moved(c, source, side, z_send.at[0], z_recv.at[c, source], x_peer)

    def r_copy(c, step):
        source = row + 2 * step
        return moved(c, source, side, r_send, z_recv.at[c, source], column(row - step))

    def two(c, shard, send, recv, peer):
        blocks = w_all.at[pl.ds(c, 2), :, shard]
        return remote(blocks, blocks, send, recv, peer)

    def x_copy(c):
        return two(c, ctx, x_send, x_recv.at[c // 2], x_peer)

    def x_arrival(c):
        return two(c, 2 * row + 1 - side, x_send, x_recv.at[c // 2], x_peer)

    def f_copy(c, source):
        return moved(c, source, side, f_send.at[source], f_recv.at[c], x_peer)

    def f_arrivals(c):
        blocks = w_all.at[c, :, 0:last]
        return remote(blocks, blocks, x_send, f_recv.at[c], x_peer)

    def sent(count, semaphore):
        blocks = w_all.at[0:count, :, 0]
        return remote(blocks, blocks, semaphore, x_recv.at[0], x_peer)

    def g_copy(c):
        return moved(c, row, 1 - side, g_send, f_recv.at[c], column(partner))

    def inner(r):
        return jnp.logical_and(r > 0, r < last)

    def first_by_z(r):
        return jnp.where(inner(r), INNER, OUTER)

    def by_z(c, r):
        return c >= first_by_z(r)

    def over_x(c, source):
        return jnp.logical_or(jnp.logical_not(by_z(c, row)), source != partner)

    def o_copy(c, h):
        return remote(stage.at[c, h], out.at[y, c, h], o_send, o_recv, y_peer)

    def send_own(c):
        for index, (distance, step) in enumerate(hops):
            @pl.when(exists(row + step * distance))
            def _():
                z_copy(c, index).start()

        @pl.when(lax.rem(c, 2) == 0)
        def _():
            x_copy(c).start()

    loads[0].wait()
    loads[1].wait()
    keys_by_head = jnp.swapaxes(wk_raw[...], 0, 1)
    values_by_head = jnp.swapaxes(wv_raw[...], 0, 1)
    for c in range(chunk_count):
        for h in range(PAIR):
            w_all[c, h, ctx, :, :nope] = keys_by_head[c * PAIR + h]
            w_all[c, h, ctx, :, nope:] = values_by_head[c * PAIR + h]

    pl.semaphore_wait(barrier, arrivals)
    for c in range(AHEAD):
        send_own(c)

    loads[2].wait()
    loads[3].wait()
    columns = jnp.transpose(
        scales[...].astype(jnp.float32).reshape(page_count * group_count, page)
    )
    for p in range(page_count):
        for g in range(group_count):
            part = pl.ds(g * group_width, group_width)
            at = p * group_count + g
            codes = pages[p, :, part].astype(jnp.float32)
            k_all[y, core, p, :, part] = (codes * columns[:, at : at + 1]).astype(jnp.bfloat16)
        k_all[y, core, p, :, latent_width:] = pages[p, :, latent_width:]
    k_copy.start()
    core_copy.start()
    loads[4].wait()
    slots = 2 * page_count
    slot = lax.broadcasted_iota(jnp.int32, (slots, slots), 0)
    place = lax.broadcasted_iota(jnp.int32, (slots, slots), 1)
    order = jnp.sum(jnp.where(table[...] == slot, place, 0), axis=1, keepdims=True)
    t_own[...] = jnp.broadcast_to(order * page - (length_in[0] - span), t_own.shape)
    t_copy.start()

    def send_queries(c, carry):
        q_copy(c).start()
        return carry

    lax.fori_loop(0, chunk_count, send_queries, 0)
    loads[5].wait()

    def settle():
        t_copy.wait_recv()
        core_copy.wait_recv()
        relay_copy.wait_recv()
        offset = lax.broadcasted_iota(jnp.int32, (page, span), 0)
        offset = offset - lax.broadcasted_iota(jnp.int32, (page, span), 1)
        for request, t_ref in ((y, t_own), (1 - y, t_rx)):
            rot[request] = k_all[request, :, :, :, latent_width:].reshape(key_count, rope)
            behind = jnp.concatenate([t_ref[p : p + 1] + offset for p in range(slots)], axis=0)
            late[request] = jnp.where(behind <= 0, 0.0, NEGATIVE)

    def attend(c, h, request, q_ref):
        latent = k_all[request, :, :, :, :latent_width].reshape(key_count, latent_width)
        weight = w_all[c, h].reshape(latent_width, -1)
        up = jnp.dot(latent, weight, preferred_element_type=jnp.float32).astype(jnp.bfloat16)
        keys = jnp.concatenate([up[:, :nope], rot[request]], axis=1)
        scores = jnp.dot(keys, q_ref[c, h], preferred_element_type=jnp.float32)
        scores = scores * scale + late[request]
        top = jnp.max(scores, axis=0, keepdims=True)
        raw = jnp.exp2(scores - top)
        total = jnp.sum(raw, axis=0, keepdims=True)
        summed = lax.dot_general(
            up[:, nope:], raw.astype(jnp.bfloat16), (((0,), (0,)), ((), ())),
            preferred_element_type=jnp.float32,
        )
        return jnp.transpose((summed * (1.0 / total)).astype(jnp.bfloat16))

    def pass_on(c, distance):
        for step in (1, -1):
            source = row + step * distance

            @pl.when(exists(source))
            def _():
                z_arrival(c, source).wait_recv()
                if distance == 2:
                    @pl.when(exists(row - step))
                    def _():
                        r_copy(c, step).start()

                @pl.when(over_x(c, source))
                def _():
                    f_copy(c, source).start()

    def advance(c, carry):
        sending = c < chunk_count
        ready = c >= LAG
        b = jnp.maximum(c - LAG, 0)
        for unit in range(2 * PAIR):
            if unit == 0:
                @pl.when(sending)
                def _():
                    pass_on(c, 1)

            if unit == 1:
                @pl.when(sending)
                def _():
                    pass_on(c, 2)
                    @pl.when(lax.rem(c, 2) == 0)
                    def _():
                        x_arrival(c).wait_recv()

                    @pl.when(by_z(c, partner))
                    def _():
                        g_copy(c).start()


            if unit == 0:
                @pl.when(c == LAG)
                def _():
                    settle()

            @pl.when(ready)
            def _():
                if unit == 0:
                    f_arrivals(b).wait_recv()
                    q_copy(b).wait_recv()
                h = unit % PAIR
                if unit < PAIR:
                    stage[b, h] = attend(b, h, 1 - y, q_rx)
                    o_copy(b, h).start()
                else:
                    out[y, b, h] = attend(b, h, y, q_own)

        @pl.when(sending)
        def _():
            pass_on(c, 3)

        @pl.when(c + AHEAD < chunk_count)
        def _():
            send_own(c + AHEAD)

        @pl.when(c == LAG - 1)
        def _():
            k_copy.wait_recv()
            relay_copy.start()

        return carry

    lax.fori_loop(0, chunk_count + LAG, advance, 0)
    k_copy.wait_send()
    t_copy.wait_send()
    core_copy.wait_send()
    relay_copy.wait_send()

    q_all = q_in.at[1 - y]
    remote(q_all, q_all, q_send, q_recv.at[0], y_peer).wait_send()
    sent(chunk_count, x_send).wait_send()
    for inside, first in ((True, INNER), (False, OUTER)):
        @pl.when(inner(partner) == inside)
        def _():
            sent(chunk_count - first, g_send).wait_send()

    for index, (distance, step) in enumerate(hops):
        @pl.when(exists(row + step * distance))
        def _():
            sent(chunk_count, z_send.at[index]).wait_send()

        if distance == 2:
            @pl.when(jnp.logical_and(exists(row + 2 * step), exists(row - step)))
            def _():
                sent(chunk_count, r_send).wait_send()

    for d in range(1, shard_columns):
        other = lax.rem(row + d, shard_columns)

        for inside, first in ((True, INNER), (False, OUTER)):
            if first > 0:
                @pl.when(jnp.logical_and(other == partner, inner(row) == inside))
                def _():
                    sent(first, f_send.at[other]).wait_send()

        @pl.when(other != partner)
        def _():
            sent(chunk_count, f_send.at[other]).wait_send()

    remote(stage, out.at[y], o_send, o_recv, y_peer).wait()


def shared_on_device(
    shards, queries, latent_pages, page_scales, page_table, lengths, w_keys, w_values
):
    _, span, heads, _ = queries.shape
    latent_rows, _, nope = w_keys.shape
    _, slots, page, width = latent_pages.shape
    latent_width = latent_rows * shards
    rope = width - latent_width
    groups = page_scales.shape[2]
    chunks = heads // (2 * PAIR)
    pool = page_table.shape[1]
    columns = shards // 2
    half = heads // 2
    q_in = jnp.transpose(queries[0], (1, 2, 0)).reshape(2, chunks, PAIR, -1, span)
    operands = (
        q_in, latent_pages[0], page_scales[0], page_table, w_keys, w_values
    )
    dma, vmem = pltpu.SemaphoreType.DMA, pltpu.VMEM
    bf16, int32 = jnp.bfloat16, jnp.int32
    out = pl.pallas_call(
        functools.partial(gather_attend, columns),
        out_shape=vmem((2, chunks, PAIR, span, nope), bf16),
        in_specs=[pl.BlockSpec(memory_space=pltpu.HBM)] * 6
        + [pl.BlockSpec(memory_space=pltpu.SMEM)],
        out_specs=pl.BlockSpec(memory_space=vmem),
        scratch_shapes=[
            vmem(q_in.shape[1:], bf16),
            vmem(q_in.shape[1:], bf16),
            vmem((2, 2, slots, page, width), bf16),
            vmem((slots, page, width), bf16),
            vmem((slots, groups, page), bf16),
            vmem((1, pool), int32),
            vmem((pool, span), int32),
            vmem((pool, span), int32),
            vmem((latent_rows, half, nope), bf16),
            vmem((latent_rows, half, nope), bf16),
            vmem((chunks, PAIR, shards, latent_rows, 2 * nope), bf16),
            vmem((2, pool * page, rope), bf16),
            vmem((2, pool * page, span), jnp.float32),
            vmem((chunks, PAIR, span, nope), bf16),
            dma((6,)), dma, dma, dma, dma, dma, dma, dma, dma,
            dma, dma((chunks,)),
            dma((4,)), dma((chunks, columns)),
            dma, dma((chunks,)),
            dma((columns,)), dma((chunks,)),
            dma, dma, dma, dma,
        ],
        compiler_params=pltpu.CompilerParams(
            collective_id=0, has_side_effects=True, vmem_limit_bytes=48 * 1024 * 1024
        ),
    )(*(pltpu.with_memory_space_constraint(x, pltpu.HBM) for x in operands), lengths)
    return jnp.swapaxes(out.reshape(heads, span, nope), 0, 1)[None]


def body_for(mesh, queries, latent_pages, page_scales, page_table, lengths, w_keys, w_values):
    args = (queries, latent_pages, page_scales, page_table, lengths, w_keys, w_values)
    shards = mesh.shape["ctx"]
    rope = latent_pages.shape[3] - w_keys.shape[0] * shards
    fits = (
        mesh.shape["groups"] == 2 and mesh.shape["head"] == 2 and shards == 8
        and w_keys.shape[0] % 16 == 0 and queries.shape[2] % 16 == 0
        and w_keys.shape == w_values.shape and 2 * rope == w_keys.shape[2]
    )
    if fits:
        return shared_on_device(shards, *args)
    return on_device(*args)


def solution(mesh):
    return jax.shard_map(
        functools.partial(body_for, mesh),
        mesh=mesh,
        in_specs=(
            P(("groups", "ctx"), None, "head", None),
            P(("groups", "ctx"), "head", None, None),
            P(("groups", "ctx"), "head", None, None),
            P(("groups", "ctx"), None),
            P(("groups", "ctx")),
            P("ctx", "head", None),
            P("ctx", "head", None),
        ),
        out_specs=P(("groups", "ctx"), None, "head", None),
        check_vma=False,
    )
```
